512 devices in a mesh: rep: 8 (over x_hi, y), grp: 64 (over x_lo, z, core).
Axes of the slice: x: 4 (x_hi: 2, x_lo: 2; x = x_hi * 2 + x_lo), y: 4, z: 16, core: 2. Of those that a mesh axis runs over, the one named last changes fastest.
Arguments:
- layer_inputs: bfloat16 [16384, 3584], P('grp'), may hold values from -32 to 32
- loss_adjoint_matrix: bfloat16 [16384, 3584], P('grp'), may hold values from -0.1875 to 0.1875
- attention_projection_matrix: bfloat16 [3584, 768], P(('rep', 'grp')), may hold values from -0.09375 to 0.09375
- merge_projection_transposed: bfloat16 [3584, 512], P(('rep', 'grp')), may hold values from -0.25 to 0.25
- packed_sequence_labels: int32 [64, 256], P('grp'), may hold values from 0 to 3, never falling along the last dimension, each value on 1 to 128 neighbouring positions
- dropout_factors: bfloat16 [8, 16384, 4, 256], P('rep', 'grp'), may hold values from -0.75 to 0.75
- straggler_filter: int32 [8, 64], P(None, 'grp'), may hold values from 0 to 1, as said below
Outputs:
- gradient: float32 [3584, 1280], P(('rep', 'grp'))
The draws below stay inside these ranges and needn't reach their ends.
Inputs may be any that keep to these rules, and one draw needn't show every extreme that they name: `straggler_filter`: each column (partition) holds exactly one 1, the surviving replica; all other entries are 0.
All inputs are finite; a program needn't handle non-finite values.
Results may differ from the reference program's by a relative error of at most 0.008.
The reference program's roundings to bfloat16 on the way (of `dropped`, `attended`, `attn_grad`, `val_grad` and `score_grad`) count: a program that leaves them out, or rounds other values in their place, can miss the bound.
Values may be sent and summed in bfloat16 or wider, within the bound.
A program may use at most 64 MiB of HBM per device.

```python
import math
import jax
import jax.numpy as jnp
import numpy as np
from jax import lax

D = 3584
HD = 128
HQ = 4
SEQ = 256
TOKENS = 16384
N_REP = 8
N_GRP = 64


def draw_layer_inputs(key, part):
    normal_part = jax.random.truncated_normal(key, -6.0, 6.0, (TOKENS, D), jnp.float32)
    return normal_part.astype(jnp.bfloat16)


def draw_straggler_filter(key, part):
    chosen = jax.random.randint(jax.random.fold_in(key, 5), (N_GRP,), 0, N_REP)
    return (jnp.arange(N_REP)[:, None] == chosen[None, :]).astype(jnp.int32)


def block_scale(stream_key, dims, split, smallest, largest):
    def one(dim, blocks):
        draws = jax.random.uniform(jax.random.fold_in(jax.random.fold_in(stream_key, 6), dim), (blocks,), jnp.float32, smallest / len(split), largest / len(split))
        return jnp.repeat(jnp.exp(draws), dims[dim] // blocks).reshape((-1,) + (1,) * (len(dims) - dim - 1))

    factor_of = one(*split[0])
    for cut in split[1:]:
        factor_of = factor_of * one(*cut)
    return factor_of


def length_profile(number_of, total, reach, skew):
    portions = [(1 << 20) // math.isqrt(rank ** skew) + 1 for rank in range(2, number_of + 1)]
    rest, given = total - reach - (number_of - 1), [1] * (number_of - 1)
    while rest > 0:
        free = [i for i in range(number_of - 1) if given[i] < reach]
        whole, left = sum([portions[i] for i in free]), rest
        for i in free:
            more = min(reach - given[i], max(1, left * portions[i] // whole), rest)
            given[i] = given[i] + more
            rest = rest - more
    return np.array([reach] + given)


def uneven(own_key, number_of, total, limit, skew):
    if number_of == 2:
        one = jax.random.randint(own_key, (), max(1, total - limit), min(limit, total - 1) + 1)
        return jnp.stack([one, total - one])
    tallies = jnp.asarray(length_profile(number_of, total, limit, skew), jnp.int32)
    twos = (number_of - 1) // 2
    donor, sink = tallies[1:1 + 2 * twos:2], tallies[2:2 + 2 * twos:2]
    slack = jnp.minimum(donor - 1, limit - sink)
    moved = jax.random.randint(jax.random.fold_in(own_key, 1), (twos,), 0, 1 << 20) % (slack + 1)
    tallies = tallies.at[1:1 + 2 * twos:2].set(donor - moved).at[2:2 + 2 * twos:2].set(sink + moved)
    return tallies[jax.random.permutation(jax.random.fold_in(own_key, 2), number_of)]


def centred(rng, extent, width, reach, shards=(), kind=jnp.bfloat16):
    drawn = width * jax.random.normal(rng, extent, jnp.float32)
    if shards:
        drawn = drawn * block_scale(rng, extent, shards, -0.22, 0.18)
    return jnp.clip(drawn, -reach, reach).astype(kind)


def setup_inputs(seed: int = 0) -> dict:
    streams_of = jax.random.split(jax.random.key(seed), 8)
    layer_inputs = draw_layer_inputs(jax.random.fold_in(streams_of[7], 71), 0)
    loss_adjoint_matrix = centred(streams_of[1], (TOKENS, D), (4.0 / TOKENS ** 0.5), 0.1875, ((0, 64),))
    attention_projection_matrix = centred(streams_of[2], (D, (HQ + 2) * HD), D ** -0.5, 0.09375, ((0, 512),))
    merge_projection_transposed = centred(streams_of[3], (D, HQ * HD), (HQ * HD) ** -0.5, 0.25, ((0, 512),))
    packed_sequence_labels = jax.vmap(lambda own: jnp.searchsorted(jnp.cumsum(uneven(own, 4, SEQ, SEQ // 2, 1)), jnp.arange(SEQ), side="right"))(jax.random.split(streams_of[4], N_GRP)).reshape((N_GRP, SEQ)).astype(jnp.int32)
    dropout_factors = centred(streams_of[5], (N_REP, TOKENS, HQ, SEQ), 0.3, 0.75, ((0, 8), (1, 64)))
    straggler_filter = draw_straggler_filter(jax.random.fold_in(streams_of[7], 71), 0)
    return dict(layer_inputs=layer_inputs, loss_adjoint_matrix=loss_adjoint_matrix, attention_projection_matrix=attention_projection_matrix, merge_projection_transposed=merge_projection_transposed, packed_sequence_labels=packed_sequence_labels, dropout_factors=dropout_factors, straggler_filter=straggler_filter)


def head_grads(hidden_rows, cot_rows, attention_projection_matrix, merge_projection_transposed, doc_row, noise_rows):
    score_scale = 1.0 / jnp.sqrt(jnp.float32(HD))
    projected = jnp.dot(hidden_rows, attention_projection_matrix, preferred_element_type=jnp.float32).astype(jnp.bfloat16)
    queries = projected[:, :HQ * HD]
    key_rows = projected[:, HQ * HD:(HQ + 1) * HD]
    val_rows = projected[:, (HQ + 1) * HD:]
    query_heads = queries.reshape(SEQ, HQ, HD).astype(jnp.float32)
    keys_wide = key_rows.astype(jnp.float32)
    vals_wide = val_rows.astype(jnp.float32)
    position = jnp.arange(SEQ, dtype=jnp.int32)
    allowed = (doc_row[:, None] == doc_row[None, :]) & (position[None, :] <= position[:, None])
    scores = jnp.einsum('ihd,jd->hij', query_heads, keys_wide) * score_scale
    scores = jnp.where(allowed[None], scores, -jnp.inf)
    highest = lax.optimization_barrier(jnp.max(scores, axis=2, keepdims=True))
    expon = jnp.exp(scores - highest)
    attn_probs = expon / lax.optimization_barrier(jnp.sum(expon, axis=2, keepdims=True))
    factor = 1.0 + jnp.transpose(noise_rows.astype(jnp.float32), (1, 0, 2))
    dropped = (attn_probs * factor).astype(jnp.bfloat16)
    dropped_wide = dropped.astype(jnp.float32)
    attended = jnp.einsum('hij,jd->ihd', dropped_wide, vals_wide).astype(jnp.bfloat16).reshape(SEQ, HQ * HD)
    attn_grad = jnp.dot(cot_rows, merge_projection_transposed, preferred_element_type=jnp.float32).astype(jnp.bfloat16)
    grad_heads = attn_grad.reshape(SEQ, HQ, HD).astype(jnp.float32)
    val_grad = jnp.einsum('hij,ihd->jd', dropped_wide, grad_heads).astype(jnp.bfloat16)
    prob_grad = jnp.einsum('ihd,jd->hij', grad_heads, vals_wide) * factor
    inner = lax.optimization_barrier(jnp.sum(attn_probs * prob_grad, axis=2, keepdims=True))
    score_grad = (attn_probs * (prob_grad - inner) * score_scale).astype(jnp.bfloat16)
    score_wide = score_grad.astype(jnp.float32)
    query_grad = jnp.einsum('hij,jd->ihd', score_wide, keys_wide).astype(jnp.bfloat16).reshape(SEQ, HQ * HD)
    key_grad = jnp.einsum('hij,ihd->jd', score_wide, query_heads).astype(jnp.bfloat16)
    stacked = jnp.concatenate([query_grad, key_grad, val_grad], axis=1)
    proj_grad = jnp.dot(hidden_rows.T, stacked, preferred_element_type=jnp.float32)
    out_grad = jnp.dot(cot_rows.T, attended, preferred_element_type=jnp.float32)
    return jnp.concatenate([proj_grad, out_grad], axis=1)

def reference(layer_inputs, loss_adjoint_matrix, attention_projection_matrix, merge_projection_transposed, packed_sequence_labels, dropout_factors, straggler_filter):
    hidden_pieces = layer_inputs.reshape(N_GRP, SEQ, D)
    cotangent_pieces = loss_adjoint_matrix.reshape(N_GRP, SEQ, D)
    noise_pieces = jnp.transpose(dropout_factors.reshape(N_REP, N_GRP, SEQ, HQ, SEQ), (1, 0, 2, 3, 4))
    kept_worker_position = lax.optimization_barrier(jnp.sum(jnp.arange(N_REP, dtype=jnp.int32)[:, None] * straggler_filter, axis=0)).astype(jnp.int32)

    def loop_body(running_total, items):
        hidden_rows, cot_rows, doc_row, noise_group, chosen = items
        noise_rows = lax.dynamic_index_in_dim(noise_group, chosen, 0, keepdims=False)
        return (running_total + head_grads(hidden_rows, cot_rows, attention_projection_matrix, merge_projection_transposed, doc_row, noise_rows), None)
    initial_sum = jnp.zeros((D, (2 * HQ + 2) * HD), jnp.float32)
    running_total, unused_value = lax.scan(loop_body, initial_sum, (hidden_pieces, cotangent_pieces, packed_sequence_labels, noise_pieces, kept_worker_position))
    return running_total
```

```python
import functools

import jax
import jax.numpy as jnp
from jax import lax
from jax.experimental import pallas as pl
from jax.experimental.pallas import tpu as pltpu
from jax.sharding import PartitionSpec as P

MESH = pl.DeviceIdType.MESH
BF = jnp.bfloat16
F32 = jnp.float32
REPS = 8
NZ = 16
PIECES = 64
REACH = 4
SEQ = 256
D = 3584
HD = 128
HQ = 4
ROWS = 7
OUTC = 1280


def iota(shape, dim):
    return lax.broadcasted_iota(jnp.int32, shape, dim)


def dot(a, b, dims=((1,), (0,))):
    return lax.dot_general(a, b, (dims, ((), ())), preferred_element_type=F32)


def kernel(
    x_hbm, y_hbm, wqkv_ref, wo_ref, lab_ref, noise_hbm, filt_ref,
    out_ref,
    xb, zb, yw, sel_e, own_e, xe, ze, xo_t, yo_t, p0s, p0r, wbuf,
    nrecv, nstage, nfull, prj, kv_ref, g32, gs, r1, s2, r2, acc, s3, relay, fin, allow,
    loc, p0_send, p0_recv, nz_send, nz_recv, nf_send, nf_recv, w_send, w_recv,
    pr_send, pr_recv, r1_send, r1_recv, r2_send, r2_recv, r3_send, relay_recv, fin_recv,
):
    rep = lax.axis_index("rep")
    grp = lax.axis_index("grp")
    x_lo = grp // 32
    z = (grp // 2) % NZ
    core = grp % 2
    partner = grp + 1 - 2 * core
    beside = grp + 32 - 64 * x_lo

    def along(d):
        return lax.rem(z + (d + NZ), NZ)

    def at_z(zz):
        return x_lo * 32 + zz * 2 + core

    def rcopy(src, dst, ssem, rsem, r, g):
        return pltpu.make_async_remote_copy(
            src_ref=src, dst_ref=dst, send_sem=ssem, recv_sem=rsem,
            device_id=(r, g), device_id_type=MESH,
        )

    def mate(k):
        return lax.rem(rep + k, REPS)

    barrier = pltpu.get_barrier_semaphore()
    near = [d for s in range(1, REACH + 1) for d in (s, -s)]
    for d in near:
        pl.semaphore_signal(barrier, inc=1, device_id=(rep, at_z(along(d))), device_id_type=MESH)
    for k in range(1, REPS):
        pl.semaphore_signal(barrier, inc=1, device_id=(mate(k), grp), device_id_type=MESH)
    pl.semaphore_signal(barrier, inc=1, device_id=(rep, partner), device_id_type=MESH)
    pl.semaphore_signal(barrier, inc=1, device_id=(rep, beside), device_id_type=MESH)

    window = pl.multiple_of(128 * (3 * rep + rep // 2), 128)
    shift_own = 64 * (rep % 2)
    cx = pltpu.make_async_copy(x_hbm, xb, loc.at[0])
    cx.start()
    czx = pltpu.make_async_copy(x_hbm, zb, loc.at[1])
    czy = pltpu.make_async_copy(y_hbm, zb, loc.at[1])

    @pl.when(rep < HQ)
    def _():
        czx.start()

    @pl.when(rep >= HQ)
    def _():
        czy.start()

    cy = pltpu.make_async_copy(y_hbm.at[:, pl.ds(window, 512)], yw, loc.at[2])
    cy.start()
    cn = pltpu.make_async_copy(
        noise_hbm.at[0, pl.ds(rep * 32, 32)], nrecv.at[rep], loc.at[3]
    )
    cn.start()

    zero_row = jnp.zeros((1, 768), F32)
    wq = jnp.concatenate([wqkv_ref[...].astype(F32), zero_row], axis=0)
    wo = jnp.concatenate([wo_ref[...].astype(F32), zero_row[:, :512]], axis=0)
    lane8 = iota((8, 128), 1)
    slot = rep // 2
    for d in range(REPS):
        if d < HQ:
            chunk, kv = wq[:, 128 * d : 128 * d + 128], wq[:, 512:640]
        else:
            chunk, kv = wo[:, 128 * (d - HQ) : 128 * (d - HQ) + 128], wq[:, 640:768]
        turned = pltpu.roll(kv, lax.rem(32 * slot + 128 - 32 * (d % 4), 128), 1)
        p0s[d, 0] = chunk.astype(BF)
        p0s[d, 1] = jnp.where(lane8 // 32 == slot, turned, 0.0).astype(BF)
    p0r[rep] = p0s[rep]

    pl.semaphore_wait(barrier, len(near) + REPS - 1 + 2)

    for k in range(1, REPS):
        rcopy(p0s.at[mate(k)], p0r.at[rep], p0_send, p0_recv.at[rep], mate(k), grp).start()
    for k in range(1, REPS):
        m = mate(k)
        rcopy(
            noise_hbm.at[0, pl.ds(m * 32, 32)], nrecv.at[rep], nz_send, nz_recv.at[rep], m, grp
        ).start()

    col = iota((128, 1024), 1)
    part = col % 16
    target = 448 * (part // 8) + 7 * (col // 16) + part % 8
    target = jnp.where(part % 8 < ROWS, target, -1)

    def fill_e(b, carry):
        sel_e[pl.ds(pl.multiple_of(128 * b, 128), 128), :] = jnp.where(
            iota((128, 1024), 0) + 128 * b == target, 1.0, 0.0
        ).astype(BF)
        return carry

    lax.fori_loop(0, 7, fill_e, 0)

    for k in range(1, REPS):
        s = mate(k)
        rcopy(p0s.at[s], p0r.at[s], p0_send, p0_recv.at[s], s, grp).wait_recv()
    for t in range(4):
        wbuf[t, grp, 0:8] = p0r[2 * t, 0]
        wbuf[t, grp, 8:16] = p0r[2 * t + 1, 0]
    for half in range(2):
        total = p0r[half, 1].astype(F32)
        for b in range(1, 4):
            total = total + p0r[2 * b + half, 1].astype(F32)
        wbuf[4, grp, 8 * half : 8 * half + 8] = total.astype(BF)

    def piece(p, g):
        return rcopy(wbuf.at[:, p], wbuf.at[:, p], w_send, w_recv.at[p], rep, g)

    for s in range(REACH, 0, -1):
        piece(grp, at_z(along(s))).start()
        piece(grp, at_z(along(-s))).start()
    piece(grp, beside).start()
    piece(grp, partner).start()

    cx.wait()
    czx.wait()

    def spread(t, carry):
        lanes = pl.ds(pl.multiple_of(896 * t, 128), 896)
        xe[t] = dot(xb[:, lanes], sel_e[...]).astype(BF)
        ze[t] = dot(zb[:, lanes], sel_e[...]).astype(BF)
        return carry

    def land(d):
        p = at_z(along(d))
        piece(p, grp).wait_recv()
        return p

    def hand_on(p):
        piece(p, beside).start()
        piece(p, partner).start()

    lax.fori_loop(0, 2, spread, 0)

    p = land(-REACH)
    for s in range(REACH, 0, -1):
        piece(p, at_z(along(s))).start()
    hand_on(p)
    p = land(REACH)
    for s in range(REACH - 1, 0, -1):
        piece(p, at_z(along(-s))).start()
    hand_on(p)
    for s in range(REACH - 1, 0, -1):
        hand_on(land(-s))
        hand_on(land(s))

    cn.wait()
    for k in range(1, REPS):
        s = mate(k)
        rcopy(
            noise_hbm.at[0, pl.ds(s * 32, 32)], nrecv.at[s], nz_send, nz_recv.at[s], s, grp
        ).wait_recv()
    kept = nrecv[0].astype(F32)
    for s in range(1, REPS):
        kept = jnp.where(filt_ref[0, s] == 1, nrecv[s].astype(F32), kept)
    for h in range(HQ):
        nstage[h] = kept[:, h, :].astype(BF)
    rows_own = pl.ds(pl.multiple_of(rep * 32, 32), 32)
    for h in range(HQ):
        nfull[h, rows_own] = nstage[h]
    for k in range(1, REPS):
        rcopy(nstage, nfull.at[:, rows_own], nf_send, nf_recv.at[rep], mate(k), grp).start()

    lax.fori_loop(2, 4, spread, 0)

    for s in range(REACH + 1, 2 * REACH):
        hand_on(land(-s))
        hand_on(land(s))
    hand_on(land(-2 * REACH))

    crow = iota((512, 128), 0)
    pidx = crow // 8
    owner = ((pidx // 16) % 2) * 32 + (pidx % 16) * 2 + pidx // 32
    want = shift_own + 7 * owner + crow % 8
    want = jnp.where(crow % 8 < ROWS, want, -1)
    for b in range(4):
        own_e[:, 128 * b : 128 * b + 128] = jnp.where(
            iota((512, 128), 1) + 128 * b == want, 1.0, 0.0
        ).astype(BF)
    cy.wait()
    xo_t[...] = dot(own_e[...], xb[:, pl.ds(window, 512)], ((1,), (1,))).astype(BF)
    yo_t[...] = dot(own_e[...], yw[...], ((1,), (1,))).astype(BF)

    lab = lab_ref[...]
    qi, kj = iota((SEQ, SEQ), 0), iota((SEQ, SEQ), 1)
    lab_col = jnp.sum(jnp.where(qi == kj, lab, 0), axis=1, keepdims=True)
    allow[...] = jnp.where((lab_col == lab) & (kj <= qi), 1.0, 0.0)

    def from_beside(i, carry):
        zz = lax.rem(z + i, NZ)
        q = (1 - x_lo) * 32 + zz * 2 + core
        piece(q, grp).wait_recv()
        piece(q, partner).start()
        return carry

    lax.fori_loop(0, NZ, from_beside, 0)

    def from_partner(i, carry):
        zz = lax.rem(z + i, NZ)
        piece(zz * 2 + 1 - core, grp).wait_recv()
        piece(32 + zz * 2 + 1 - core, grp).wait_recv()
        return carry

    lax.fori_loop(0, NZ, from_partner, 0)

    own_cols = jnp.zeros((SEQ, HD), F32)
    for t in range(4):
        own_cols = own_cols + dot(ze[t], wbuf[t].reshape(1024, HD))
    lane = iota((SEQ, HD), 1) // 32
    kv_sum = jnp.zeros((SEQ, HD), F32)
    w_kv = wbuf[4].reshape(1024, HD)
    for b in range(4):
        kv_sum = jnp.where(lane == b, dot(xe[b], w_kv), kv_sum)
    kv_sum = kv_sum + pltpu.roll(kv_sum, 64, 1)
    kv_sum = kv_sum + pltpu.roll(kv_sum, 32, 1)
    lane64 = iota((64, HD), 1) // 32
    packed = kv_sum[0:64]
    for b in range(1, 4):
        packed = jnp.where(lane64 == b, kv_sum[64 * b : 64 * b + 64], packed)
    prj[rep, 0:SEQ] = own_cols.astype(BF)
    prj[rep, SEQ:320] = packed.astype(BF)
    for k in range(1, REPS):
        rcopy(prj.at[rep], prj.at[rep], pr_send, pr_recv.at[rep], mate(k), grp).start()
    for k in range(1, REPS):
        s = mate(k)
        rcopy(nstage, nfull.at[:, pl.ds(pl.multiple_of(s * 32, 32), 32)], nf_send, nf_recv.at[s], s, grp).wait_recv()
    for k in range(1, REPS):
        s = mate(k)
        rcopy(prj.at[s], prj.at[s], pr_send, pr_recv.at[s], s, grp).wait_recv()

    for which in range(2):
        parts = [prj[4 * which + r, SEQ:320].astype(F32) for r in range(4)]
        for b in range(4):
            whole = jnp.zeros((64, HD), F32)
            for r in range(4):
                turned = parts[r] if r == b else pltpu.roll(parts[r], (32 * (r - b)) % 128, 1)
                whole = jnp.where(lane64 == r, turned, whole)
            kv_ref[which, 64 * b : 64 * b + 64] = whole.astype(BF)

    scale = 1.0 / jnp.sqrt(jnp.float32(HD))
    keys, vals = kv_ref[0], kv_ref[1]
    key_grad = jnp.zeros((SEQ, HD), F32)
    val_grad = jnp.zeros((SEQ, HD), F32)

    def put(cols, product):
        g32[:, :, cols] = product.reshape(PIECES, 8, HD)

    for h in range(HQ):
        q, a = prj[h, 0:SEQ], prj[HQ + h, 0:SEQ]
        scores = dot(q, keys, ((1,), (1,))) * scale
        scores = jnp.where(allow[...] > 0.5, scores, -jnp.inf)
        expon = jnp.exp(scores - jnp.max(scores, axis=1, keepdims=True))
        probs = expon / jnp.sum(expon, axis=1, keepdims=True)
        factor = 1.0 + nfull[h].astype(F32)
        dropped = (probs * factor).astype(BF)
        attended = dot(dropped, vals).astype(BF)
        val_grad = val_grad + dot(dropped, a, ((0,), (0,)))
        prob_grad = dot(a, vals, ((1,), (1,))) * factor
        inner = jnp.sum(probs * prob_grad, axis=1, keepdims=True)
        score_grad = (probs * (prob_grad - inner) * scale).astype(BF)
        query_grad = dot(score_grad, keys).astype(BF)
        key_grad = key_grad + dot(score_grad, q, ((0,), (0,)))
        put(slice(128 * h, 128 * h + 128), dot(xo_t[...], query_grad))
        put(slice(768 + 128 * h, 896 + 128 * h), dot(yo_t[...], attended))
    put(slice(512, 640), dot(xo_t[...], key_grad.astype(BF)))
    put(slice(640, 768), dot(xo_t[...], val_grad.astype(BF)))

    theirs, mine = (1 - core) * 32, core * 32
    for i in range(2):
        xs = (1 - x_lo) if i == 0 else x_lo
        gs[i] = g32[pl.ds(theirs + xs * 16, 16)].astype(BF)
        rcopy(gs.at[i], r1.at[i], r1_send, r1_recv.at[i], rep, partner).start()

    order = [2 * REACH] + [d for s in range(2 * REACH - 1, 0, -1) for d in (s, -s)] + [0]
    rcopy(gs.at[0], r1.at[0], r1_send, r1_recv.at[0], rep, partner).wait_recv()
    s2[...] = (g32[pl.ds(mine + (1 - x_lo) * 16, 16)] + r1[0].astype(F32)).astype(BF)

    def cross(zz):
        return rcopy(s2.at[zz], r2.at[zz], r2_send, r2_recv.at[zz], rep, beside)

    for d in order:
        cross(along(d)).start()
    rcopy(gs.at[1], r1.at[1], r1_send, r1_recv.at[1], rep, partner).wait_recv()
    acc[...] = g32[pl.ds(mine + x_lo * 16, 16)] + r1[1].astype(F32)

    def hop(zz, dst, rsem, d):
        return rcopy(s3.at[zz], dst, r3_send, rsem, rep, at_z(along(d)))

    def fin_copy(zz, d):
        i = d + REACH if d < 0 else d + REACH - 1
        return hop(zz, fin.at[i], fin_recv.at[i], d)

    def relay_copy(zz, d):
        i = d + REACH - 1 if d < 0 else d + REACH - 2
        return hop(zz, relay.at[i], relay_recv.at[i], d)

    for d in order:
        zz = along(d)
        cross(zz).wait_recv()
        total = acc[zz] + r2[zz].astype(F32)
        if d == 0 or abs(d) == REACH:
            acc[zz] = total
            continue
        s3[zz] = total.astype(BF)
        if abs(d) > REACH:
            relay_copy(zz, d - REACH if d > 0 else d + REACH).start()
        else:
            fin_copy(zz, d).start()
    for sign in (1, -1):
        zz = along(sign * REACH)
        total = acc[zz]
        for s in range(REACH if sign > 0 else REACH - 1, 0, -1):
            d = sign * s
            i = d + REACH - 1 if d < 0 else d + REACH - 2
            relay_copy(zz, d).wait_recv()
            total = total + relay[i].astype(F32)
        s3[zz] = total.astype(BF)
        fin_copy(zz, sign * REACH).start()
    total = acc[z]
    for s in range(1, REACH + 1):
        for d in (s, -s):
            i = d + REACH if d < 0 else d + REACH - 1
            fin_copy(z, d).wait_recv()
            total = total + fin[i].astype(F32)
    out_ref[...] = total[0:ROWS]

    def sent(ref, sem):
        pltpu.make_async_copy(ref, ref, sem).wait()

    sent(p0s.at[pl.ds(0, 7)], p0_send)
    sent(nrecv.at[pl.ds(0, 7)], nz_send)
    for k in range(1, REPS):
        rcopy(nstage, nfull.at[:, rows_own], nf_send, nf_recv.at[rep], mate(k), grp).wait_send()
    sent(wbuf.at[:, pl.ds(0, 63)], w_send)
    sent(prj.at[pl.ds(0, 7)], pr_send)
    sent(gs, r1_send)
    sent(s2, r2_send)
    sent(s3.at[pl.ds(0, 15)], r3_send)


def per_device(x, y, wqkv, wo, lab, noise, filt):
    vm = pltpu.VMEM
    dma = pltpu.SemaphoreType.DMA
    vspec = pl.BlockSpec(memory_space=pltpu.VMEM)
    anys = pl.BlockSpec(memory_space=pl.ANY)
    return pl.pallas_call(
        kernel,
        out_shape=jax.ShapeDtypeStruct((ROWS, OUTC), F32),
        in_specs=[anys, anys, vspec, vspec, vspec, anys, pl.BlockSpec(memory_space=pltpu.SMEM)],
        out_specs=vspec,
        scratch_shapes=[
            vm((SEQ, D), BF),
            vm((SEQ, D), BF),
            vm((SEQ, 512), BF),
            vm((896, 1024), BF),
            vm((512, 512), BF),
            vm((4, SEQ, 1024), BF),
            vm((4, SEQ, 1024), BF),
            vm((512, SEQ), BF),
            vm((512, SEQ), BF),
            vm((REPS, 2, 8, 128), BF),
            vm((REPS, 2, 8, 128), BF),
            vm((5, PIECES, 16, 128), BF),
            vm((REPS, 32, HQ, SEQ), BF),
            vm((HQ, 32, SEQ), BF),
            vm((HQ, SEQ, SEQ), BF),
            vm((REPS, 320, HD), BF),
            vm((2, SEQ, HD), BF),
            vm((PIECES, 8, OUTC), F32),
            vm((2, NZ, 8, OUTC), BF),
            vm((2, NZ, 8, OUTC), BF),
            vm((NZ, 8, OUTC), BF),
            vm((NZ, 8, OUTC), BF),
            vm((NZ, 8, OUTC), F32),
            vm((NZ, 8, OUTC), BF),
            vm((2 * REACH - 1, 8, OUTC), BF),
            vm((2 * REACH, 8, OUTC), BF),
            vm((SEQ, SEQ), F32),
            dma((4,)),
            dma, dma((REPS,)),
            dma, dma((REPS,)),
            dma, dma((REPS,)),
            dma, dma((PIECES,)),
            dma, dma((REPS,)),
            dma, dma((2,)),
            dma, dma((NZ,)),
            dma, dma((2 * REACH - 1,)), dma((2 * REACH,)),
        ],
        compiler_params=pltpu.CompilerParams(
            collective_id=0, has_side_effects=True, vmem_limit_bytes=56 * 1024 * 1024
        ),
    )(x, y, wqkv, wo, lab, noise, filt.reshape(1, REPS))


def solution(mesh):
    return jax.shard_map(
        per_device,
        mesh=mesh,
        in_specs=(
            P("grp", None),
            P("grp", None),
            P(("rep", "grp"), None),
            P(("rep", "grp"), None),
            P("grp", None),
            P("rep", "grp", None, None),
            P(None, "grp"),
        ),
        out_specs=P(("rep", "grp"), None),
        check_vma=False,
    )
```

```python
import functools

import jax
import jax.numpy as jnp
from jax import lax
from jax.experimental import pallas as pl
from jax.experimental.pallas import tpu as pltpu
from jax.sharding import PartitionSpec as P

MESH = pl.DeviceIdType.MESH
BF = jnp.bfloat16
F32 = jnp.float32
REPS = 8
NZ = 16
PIECES = 64
REACH = 4
SEQ = 256
D = 3584
HD = 128
HQ = 4
ROWS = 7
OUTC = 1280


def iota(shape, dim):
    return lax.broadcasted_iota(jnp.int32, shape, dim)


def dot(a, b, dims=((1,), (0,))):
    return lax.dot_general(a, b, (dims, ((), ())), preferred_element_type=F32)


def kernel(
    x_hbm, y_hbm, wqkv_ref, wo_ref, lab_ref, noise_hbm, filt_ref,
    out_ref,
    xb, zb, yw, sel_e, own_e, xe, ze, xo_t, yo_t, p0s, p0r, wbuf,
    nhi, nband, nrecv, nstage, nfull, prj, kvp, kv_ref, allow,
    ga, gsa, r1a, s2a, r2a, acca, s3a, relaya, fina,
    gb, gsb, r1b, s2b, r2b, accb, s3b, relayb, finb,
    loc, p0_send, p0_recv, nz_send, nz_recv, nf_send, nf_recv, w_send, w_recv,
    kv_send, kv_recv, pr_send, pr_recv,
    r1_send, r1_recv, r2_send, r2_recv, r3_send, relay_recv, fin_recv,
):
    rep = lax.axis_index("rep")
    grp = lax.axis_index("grp")
    x_lo = grp // 32
    z = (grp // 2) % NZ
    core = grp % 2
    partner = grp + 1 - 2 * core
    beside = grp + 32 - 64 * x_lo

    def along(d):
        return lax.rem(z + (d + NZ), NZ)

    def at_z(zz):
        return x_lo * 32 + zz * 2 + core

    def rcopy(src, dst, ssem, rsem, r, g):
        return pltpu.make_async_remote_copy(
            src_ref=src, dst_ref=dst, send_sem=ssem, recv_sem=rsem,
            device_id=(r, g), device_id_type=MESH,
        )

    def mate(k):
        return lax.rem(rep + k, REPS)

    barrier = pltpu.get_barrier_semaphore()
    near = [d for s in range(REACH, 0, -1) for d in (s, -s)]
    for k in range(1, REPS):
        pl.semaphore_signal(barrier, inc=1, device_id=(mate(k), grp), device_id_type=MESH)
    for d in near:
        pl.semaphore_signal(barrier, inc=1, device_id=(rep, at_z(along(d))), device_id_type=MESH)
    pl.semaphore_signal(barrier, inc=1, device_id=(rep, partner), device_id_type=MESH)
    pl.semaphore_signal(barrier, inc=1, device_id=(rep, beside), device_id_type=MESH)

    window = pl.multiple_of(128 * (3 * rep + rep // 2), 128)
    shift_own = 64 * (rep % 2)
    cnh = pltpu.make_async_copy(noise_hbm.at[0, pl.ds(128, 128)], nhi, loc.at[3])
    cnh.start()
    cnl = pltpu.make_async_copy(
        noise_hbm.at[0, pl.ds(0, 128), :, pl.ds(0, 128)], nband.at[pl.ds(0, 128)], loc.at[4]
    )
    cnl.start()
    cx = pltpu.make_async_copy(x_hbm, xb, loc.at[0])
    cx.start()
    czx = pltpu.make_async_copy(x_hbm, zb, loc.at[1])
    czy = pltpu.make_async_copy(y_hbm, zb, loc.at[1])

    @pl.when(rep < HQ)
    def _():
        czx.start()

    @pl.when(rep >= HQ)
    def _():
        czy.start()

    cy = pltpu.make_async_copy(y_hbm.at[:, pl.ds(window, 512)], yw, loc.at[2])
    cy.start()

    zero_row = jnp.zeros((1, 768), F32)
    wq = jnp.concatenate([wqkv_ref[...].astype(F32), zero_row], axis=0)
    wo = jnp.concatenate([wo_ref[...].astype(F32), zero_row[:, :512]], axis=0)
    lane8 = iota((8, 128), 1)
    slot = rep // 2
    for d in range(REPS):
        if d < HQ:
            chunk, kv = wq[:, 128 * d : 128 * d + 128], wq[:, 512:640]
        else:
            chunk, kv = wo[:, 128 * (d - HQ) : 128 * (d - HQ) + 128], wq[:, 640:768]
        turned = pltpu.roll(kv, lax.rem(32 * slot + 128 - 32 * (d % 4), 128), 1)
        p0s[d, 0] = chunk.astype(BF)
        p0s[d, 1] = jnp.where(lane8 // 32 == slot, turned, 0.0).astype(BF)
    p0r[rep] = p0s[rep]

    pl.semaphore_wait(barrier, len(near) + REPS - 1 + 2)

    for k in range(1, REPS):
        rcopy(p0s.at[mate(k)], p0r.at[rep], p0_send, p0_recv.at[rep], mate(k), grp).start()

    cnh.wait()

    def band(i, carry):
        rows = pl.ds(pl.multiple_of(16 * i, 16), 16)
        low = nhi[rows, :, 0:128].astype(F32)
        high = nhi[rows, :, 128:256].astype(F32)
        keep = iota((16, HQ, 128), 2) > iota((16, HQ, 128), 0) + 16 * i
        nband[pl.ds(pl.multiple_of(128 + 16 * i, 16), 16)] = jnp.where(keep, low, high).astype(BF)
        return carry

    lax.fori_loop(0, 8, band, 0)
    cnl.wait()

    def slice_of(r):
        return nband.at[pl.ds(pl.multiple_of(r * 32, 32), 32)]

    for k in range(1, REPS):
        rcopy(slice_of(mate(k)), nrecv.at[rep], nz_send, nz_recv.at[rep], mate(k), grp).start()
    nrecv[rep] = nband[pl.ds(pl.multiple_of(rep * 32, 32), 32)]

    col = iota((128, 1024), 1)
    part = col % 16
    target = 448 * (part // 8) + 7 * (col // 16) + part % 8
    target = jnp.where(part % 8 < ROWS, target, -1)

    def fill_e(b, carry):
        sel_e[pl.ds(pl.multiple_of(128 * b, 128), 128), :] = jnp.where(
            iota((128, 1024), 0) + 128 * b == target, 1.0, 0.0
        ).astype(BF)
        return carry

    lax.fori_loop(0, 7, fill_e, 0)

    for k in range(1, REPS):
        s = mate(k)
        rcopy(p0s.at[s], p0r.at[s], p0_send, p0_recv.at[s], s, grp).wait_recv()
    for t in range(4):
        wbuf[t, grp, 0:8] = p0r[2 * t, 0]
        wbuf[t, grp, 8:16] = p0r[2 * t + 1, 0]
    for half in range(2):
        total = p0r[half, 1].astype(F32)
        for b in range(1, 4):
            total = total + p0r[2 * b + half, 1].astype(F32)
        wbuf[4, grp, 8 * half : 8 * half + 8] = total.astype(BF)

    def piece(p, g):
        return rcopy(wbuf.at[:, p], wbuf.at[:, p], w_send, w_recv.at[p], rep, g)

    for d in near:
        piece(grp, at_z(along(d))).start()
    piece(grp, beside).start()
    piece(grp, partner).start()

    cx.wait()
    czx.wait()

    def spread(t):
        lanes = pl.ds(pl.multiple_of(896 * t, 128), 896)

        xe[t] = dot(xb[:, lanes], sel_e[...]).astype(BF)
        ze[t] = dot(zb[:, lanes], sel_e[...]).astype(BF)

    def land(d):
        p = at_z(along(d))
        piece(p, grp).wait_recv()
        return p

    def hand_on(p):
        piece(p, beside).start()
        piece(p, partner).start()

    spread(0)

    p = land(-REACH)
    for s in range(REACH, 0, -1):
        piece(p, at_z(along(s))).start()
    hand_on(p)
    p = land(REACH)
    for s in range(REACH - 1, 0, -1):
        piece(p, at_z(along(-s))).start()
    hand_on(p)
    for s in range(1, REACH):
        hand_on(land(-s))
        hand_on(land(s))

    spread(1)

    for k in range(1, REPS):
        s = mate(k)
        rcopy(slice_of(s), nrecv.at[s], nz_send, nz_recv.at[s], s, grp).wait_recv()
    kept = nrecv[0].astype(F32)
    for s in range(1, REPS):
        kept = jnp.where(filt_ref[0, s] == 1, nrecv[s].astype(F32), kept)
    rows_own = pl.ds(pl.multiple_of(rep * 32, 32), 32)
    for h in range(HQ):
        rows = kept[:, h, :].astype(BF)
        nstage[h] = rows
        nfull[h, rows_own] = rows
    for k in range(1, REPS):
        rcopy(nstage, nfull.at[:, rows_own], nf_send, nf_recv.at[rep], mate(k), grp).start()

    spread(2)
    spread(3)

    for s in range(REACH + 1, 2 * REACH):
        hand_on(land(-s))
        hand_on(land(s))
    hand_on(land(-2 * REACH))

    outward = [0] + [d for s in range(1, 2 * REACH) for d in (-s, s)] + [2 * REACH]
    for d in outward:
        q = (1 - x_lo) * 32 + along(d) * 2 + core
        piece(q, grp).wait_recv()
        piece(q, partner).start()

    def from_partner(side):
        def one(i, carry):
            piece(side * 32 + lax.rem(z + i, NZ) * 2 + 1 - core, grp).wait_recv()
            return carry

        lax.fori_loop(0, NZ, one, 0)

    lane = iota((SEQ, HD), 1) // 32

    def kv_part(side):
        w = wbuf[4, pl.ds(side * 32, 32)].reshape(512, HD)
        lanes = pl.ds(pl.multiple_of(512 * side, 128), 512)
        total = jnp.zeros((SEQ, HD), F32)
        for b in range(4):
            total = jnp.where(lane == b, dot(xe[b, :, lanes], w), total)
        return total

    def own_part(side):
        lanes = pl.ds(pl.multiple_of(512 * side, 128), 512)
        total = jnp.zeros((SEQ, HD), F32)
        for t in range(4):
            total = total + dot(ze[t, :, lanes], wbuf[t, pl.ds(side * 32, 32)].reshape(512, HD))
        return total

    from_partner(x_lo)
    kv_sum = kv_part(x_lo)
    own_cols = own_part(x_lo)
    from_partner(1 - x_lo)
    kv_sum = kv_sum + kv_part(1 - x_lo)
    kv_sum = kv_sum + pltpu.roll(kv_sum, 64, 1)
    kv_sum = kv_sum + pltpu.roll(kv_sum, 32, 1)
    lane64 = iota((64, HD), 1) // 32
    packed = kv_sum[0:64]
    for b in range(1, 4):
        packed = jnp.where(lane64 == b, kv_sum[64 * b : 64 * b + 64], packed)
    kvp[rep] = packed.astype(BF)
    far_first = (2, 6, 1, 3, 5, 7, 4)
    for k in far_first:
        rcopy(kvp.at[rep], kvp.at[rep], kv_send, kv_recv.at[rep], mate(k), grp).start()
    own_cols = own_cols + own_part(1 - x_lo)
    prj[rep] = own_cols.astype(BF)
    for k in (4, 1, 3, 5, 7, 2, 6):
        rcopy(prj.at[rep], prj.at[rep], pr_send, pr_recv.at[rep], mate(k), grp).start()

    crow = iota((512, 128), 0)
    pidx = crow // 8
    owner = ((pidx // 16) % 2) * 32 + (pidx % 16) * 2 + pidx // 32
    want = shift_own + 7 * owner + crow % 8
    want = jnp.where(crow % 8 < ROWS, want, -1)
    for b in range(4):
        own_e[:, 128 * b : 128 * b + 128] = jnp.where(
            iota((512, 128), 1) + 128 * b == want, 1.0, 0.0
        ).astype(BF)
    cy.wait()
    xo_t[...] = dot(own_e[...], xb[:, pl.ds(window, 512)], ((1,), (1,))).astype(BF)
    yo_t[...] = dot(own_e[...], yw[...], ((1,), (1,))).astype(BF)

    lab = lab_ref[...]
    qi, kj = iota((SEQ, SEQ), 0), iota((SEQ, SEQ), 1)
    lab_col = jnp.sum(jnp.where(qi == kj, lab, 0), axis=1, keepdims=True)
    allow[...] = jnp.where((lab_col == lab) & (kj <= qi), 1.0, 0.0)

    for k in range(1, REPS):
        s = mate(k)
        rcopy(kvp.at[s], kvp.at[s], kv_send, kv_recv.at[s], s, grp).wait_recv()
    for which in range(2):
        parts = [kvp[4 * which + r].astype(F32) for r in range(4)]
        for b in range(4):
            whole = jnp.zeros((64, HD), F32)
            for r in range(4):
                turned = parts[r] if r == b else pltpu.roll(parts[r], (32 * (r - b)) % 128, 1)
                whole = jnp.where(lane64 == r, turned, whole)
            kv_ref[which, 64 * b : 64 * b + 64] = whole.astype(BF)
    for k in range(1, REPS):
        s = mate(k)
        rcopy(nstage, nfull.at[:, pl.ds(pl.multiple_of(s * 32, 32), 32)], nf_send, nf_recv.at[s], s, grp).wait_recv()

    scale = 1.0 / jnp.sqrt(jnp.float32(HD))
    keys, vals = kv_ref[0], kv_ref[1]
    key_grad = jnp.zeros((SEQ, HD), F32)
    val_grad = jnp.zeros((SEQ, HD), F32)

    def put(g32, at, product):
        g32[:, :, 128 * at : 128 * at + 128] = product.reshape(PIECES, 8, HD)

    heads = [lax.rem(rep + o, HQ) for o in (0, 1, 3, 2)]

    def attend(i, key_grad, val_grad):
        h = heads[i]
        if i == 0:
            s = mate(HQ)
            rcopy(prj.at[s], prj.at[s], pr_send, pr_recv.at[s], s, grp).wait_recv()
        else:
            for s in (h, HQ + h):
                rcopy(prj.at[s], prj.at[s], pr_send, pr_recv.at[s], s, grp).wait_recv()
        q, a = prj[h], prj[HQ + h]
        scores = dot(q, keys, ((1,), (1,))) * scale
        scores = jnp.where(allow[...] > 0.5, scores, -jnp.inf)
        expon = jnp.exp(scores - jnp.max(scores, axis=1, keepdims=True))
        probs = expon / jnp.sum(expon, axis=1, keepdims=True)
        factor = 1.0 + nfull[h].astype(F32)
        factor = jnp.concatenate([factor, factor], axis=1)
        dropped = (probs * factor).astype(BF)
        attended = dot(dropped, vals).astype(BF)
        val_grad = val_grad + dot(dropped, a, ((0,), (0,)))
        prob_grad = dot(a, vals, ((1,), (1,))) * factor
        inner = jnp.sum(probs * prob_grad, axis=1, keepdims=True)
        score_grad = (probs * (prob_grad - inner) * scale).astype(BF)
        query_grad = dot(score_grad, keys).astype(BF)
        key_grad = key_grad + dot(score_grad, q, ((0,), (0,)))
        g32 = ga if i < 2 else gb
        put(g32, 2 * (i % 2), dot(xo_t[...], query_grad))
        put(g32, 2 * (i % 2) + 1, dot(yo_t[...], attended))
        return key_grad, val_grad

    theirs, mine = (1 - core) * 32, core * 32
    order = [2 * REACH] + [d for s in range(2 * REACH - 1, 0, -1) for d in (s, -s)] + [0]

    def relay_at(d):
        return d + REACH - 1 if d < 0 else d + REACH - 2

    def fin_at(d):
        return d + REACH if d < 0 else d + REACH - 1

    class Sums:
        def __init__(self, n, g32, gs, r1, s2, r2, acc, s3, relay, fin):
            self.n, self.g32, self.gs, self.r1, self.s2, self.r2 = n, g32, gs, r1, s2, r2
            self.acc, self.s3, self.relay, self.fin = acc, s3, relay, fin

        def core_copy(self, i):
            return rcopy(self.gs.at[i], self.r1.at[i], r1_send.at[self.n], r1_recv.at[self.n, i], rep, partner)

        def cross(self, zz):
            return rcopy(self.s2.at[zz], self.r2.at[zz], r2_send.at[self.n], r2_recv.at[self.n, zz], rep, beside)

        def hop(self, zz, dst, rsem, d):
            return rcopy(self.s3.at[zz], dst, r3_send.at[self.n], rsem, rep, at_z(along(d)))

        def fin_copy(self, zz, d):
            return self.hop(zz, self.fin.at[fin_at(d)], fin_recv.at[self.n, fin_at(d)], d)

        def relay_copy(self, zz, d):
            return self.hop(zz, self.relay.at[relay_at(d)], relay_recv.at[self.n, relay_at(d)], d)

        def to_partner(self):
            for i in range(2):
                xs = (1 - x_lo) if i == 0 else x_lo
                self.gs[i] = self.g32[pl.ds(theirs + xs * 16, 16)].astype(BF)
                self.core_copy(i).start()

        def to_beside(self):
            self.core_copy(0).wait_recv()
            self.s2[...] = (
                self.g32[pl.ds(mine + (1 - x_lo) * 16, 16)] + self.r1[0].astype(F32)
            ).astype(BF)
            for d in order:
                self.cross(along(d)).start()
            self.core_copy(1).wait_recv()
            self.acc[...] = self.g32[pl.ds(mine + x_lo * 16, 16)] + self.r1[1].astype(F32)

        def to_z(self):
            for d in order:
                zz = along(d)
                self.cross(zz).wait_recv()
                total = self.acc[zz] + self.r2[zz].astype(F32)
                if d == 0 or abs(d) == REACH:
                    self.acc[zz] = total
                    continue
                self.s3[zz] = total.astype(BF)
                if abs(d) > REACH:
                    self.relay_copy(zz, d - REACH if d > 0 else d + REACH).start()
                else:
                    self.fin_copy(zz, d).start()

        def relays(self):
            for sign in (1, -1):
                zz = along(sign * REACH)
                total = self.acc[zz]
                for s in range(REACH if sign > 0 else REACH - 1, 0, -1):
                    self.relay_copy(zz, sign * s).wait_recv()
                    total = total + self.relay[relay_at(sign * s)].astype(F32)
                self.s3[zz] = total.astype(BF)
                self.fin_copy(zz, sign * REACH).start()

        def final(self):
            total = self.acc[z]
            for s in range(1, REACH + 1):
                for d in (s, -s):
                    self.fin_copy(z, d).wait_recv()
                    total = total + self.fin[fin_at(d)].astype(F32)
            return total

    first = Sums(0, ga, gsa, r1a, s2a, r2a, acca, s3a, relaya, fina)
    last = Sums(1, gb, gsb, r1b, s2b, r2b, accb, s3b, relayb, finb)

    key_grad, val_grad = attend(0, key_grad, val_grad)
    key_grad, val_grad = attend(1, key_grad, val_grad)
    first.to_partner()
    key_grad, val_grad = attend(2, key_grad, val_grad)
    first.to_beside()
    key_grad, val_grad = attend(3, key_grad, val_grad)
    put(gb, 4, dot(xo_t[...], key_grad.astype(BF)))
    put(gb, 5, dot(xo_t[...], val_grad.astype(BF)))
    last.to_partner()
    last.to_beside()
    first.to_z()
    first.relays()
    last.to_z()
    last.relays()

    def write(total, at, lanes):
        out_ref[:, lanes] = total[0:ROWS, 128 * at : 128 * at + 128]

    for group, total in ((0, first.final()), (1, last.final())):
        for i in range(2):
            h = heads[2 * group + i]
            write(total, 2 * i, pl.ds(pl.multiple_of(128 * h, 128), 128))
            write(total, 2 * i + 1, pl.ds(pl.multiple_of(768 + 128 * h, 128), 128))
        if group == 1:
            write(total, 4, pl.ds(512, 128))
            write(total, 5, pl.ds(640, 128))

    def sent(ref, sem):
        pltpu.make_async_copy(ref, ref, sem).wait()

    sent(p0s.at[pl.ds(0, 7)], p0_send)
    sent(nrecv.at[pl.ds(0, 7)], nz_send)
    for k in range(1, REPS):
        rcopy(nstage, nfull.at[:, rows_own], nf_send, nf_recv.at[rep], mate(k), grp).wait_send()
    sent(wbuf.at[:, pl.ds(0, 63)], w_send)
    sent(kvp.at[pl.ds(0, 7)], kv_send)
    sent(prj.at[pl.ds(0, 7)], pr_send)
    for g in (first, last):
        sent(g.gs, r1_send.at[g.n])
        sent(g.s2, r2_send.at[g.n])
        sent(g.s3.at[pl.ds(0, 15)], r3_send.at[g.n])


def per_device(x, y, wqkv, wo, lab, noise, filt):
    vm = pltpu.VMEM
    dma = pltpu.SemaphoreType.DMA
    vspec = pl.BlockSpec(memory_space=pltpu.VMEM)
    anys = pl.BlockSpec(memory_space=pl.ANY)
    return pl.pallas_call(
        kernel,
        out_shape=jax.ShapeDtypeStruct((ROWS, OUTC), F32),
        in_specs=[anys, anys, vspec, vspec, vspec, anys, pl.BlockSpec(memory_space=pltpu.SMEM)],
        out_specs=vspec,
        scratch_shapes=[
            vm((SEQ, D), BF),
            vm((SEQ, D), BF),
            vm((SEQ, 512), BF),
            vm((896, 1024), BF),
            vm((512, 512), BF),
            vm((4, SEQ, 1024), BF),
            vm((4, SEQ, 1024), BF),
            vm((512, SEQ), BF),
            vm((512, SEQ), BF),
            vm((REPS, 2, 8, 128), BF),
            vm((REPS, 2, 8, 128), BF),
            vm((5, PIECES, 16, 128), BF),
            vm((128, HQ, SEQ), BF),
            vm((SEQ, HQ, 128), BF),
            vm((REPS, 32, HQ, 128), BF),
            vm((HQ, 32, 128), BF),
            vm((HQ, SEQ, 128), BF),
            vm((REPS, SEQ, HD), BF),
            vm((REPS, 64, HD), BF),
            vm((2, SEQ, HD), BF),
            vm((SEQ, SEQ), F32),
        ]
        + [
            s
            for width in (512, 768)
            for s in (
                vm((PIECES, 8, width), F32),
                vm((2, NZ, 8, width), BF),
                vm((2, NZ, 8, width), BF),
                vm((NZ, 8, width), BF),
                vm((NZ, 8, width), BF),
                vm((NZ, 8, width), F32),
                vm((NZ, 8, width), BF),
                vm((2 * REACH - 1, 8, width), BF),
                vm((2 * REACH, 8, width), BF),
            )
        ]
        + [
            dma((5,)),
            dma, dma((REPS,)),
            dma, dma((REPS,)),
            dma, dma((REPS,)),
            dma, dma((PIECES,)),
            dma, dma((REPS,)),
            dma, dma((REPS,)),
            dma((2,)), dma((2, 2)),
            dma((2,)), dma((2, NZ)),
            dma((2,)), dma((2, 2 * REACH - 1)), dma((2, 2 * REACH)),
        ],
        compiler_params=pltpu.CompilerParams(
            collective_id=0, has_side_effects=True, vmem_limit_bytes=56 * 1024 * 1024
        ),
    )(x, y, wqkv, wo, lab, noise, filt.reshape(1, REPS))


def solution(mesh):
    return jax.shard_map(
        per_device,
        mesh=mesh,
        in_specs=(
            P("grp", None),
            P("grp", None),
            P(("rep", "grp"), None),
            P(("rep", "grp"), None),
            P("grp", None),
            P("rep", "grp", None, None),
            P(None, "grp"),
        ),
        out_specs=P(("rep", "grp"), None),
        check_vma=False,
    )
```

```python
import functools

import jax
import jax.numpy as jnp
from jax import lax
from jax.experimental import pallas as pl
from jax.experimental.pallas import tpu as pltpu
from jax.sharding import PartitionSpec as P

MESH = pl.DeviceIdType.MESH
BF = jnp.bfloat16
F32 = jnp.float32
REPS = 8
NZ = 16
PIECES = 64
REACH = 4
SEQ = 256
D = 3584
HD = 128
HQ = 4
ROWS = 7
OUTC = 1280


def iota(shape, dim):
    return lax.broadcasted_iota(jnp.int32, shape, dim)


def dot(a, b, dims=((1,), (0,))):
    return lax.dot_general(a, b, (dims, ((), ())), preferred_element_type=F32)


def kernel(
    x_hbm, y_hbm, wqkv_hbm, wo_hbm, lab_hbm, noise_hbm, filt_hbm,
    out_ref, wqkv_ref, wo_ref, lab_ref, filt_ref,
    xb, zb, yw, sel_e, own_e, xe, ze, xo_t, yo_t, p0s, p0r, wbuf,
    nhi, nband, nrecv, nstage, nfull, prj, kvp, kv_ref, allow,
    g_0, gs_0, r1_0, s2_0, r2_0, acc_0, s3_0, relay_0, fin_0,
    g_1, gs_1, r1_1, s2_1, r2_1, acc_1, s3_1, relay_1, fin_1,
    g_2, gs_2, r1_2, s2_2, r2_2, acc_2, s3_2, relay_2, fin_2,
    loc, p0_send, p0_recv, nz_send, nz_recv, nf_send, nf_recv, w_send, w_recv,
    kv_send, kv_recv, pr_send, pr_recv,
    r1_send, r1_recv, r2_send, r2_recv, r3_send, relay_recv, fin_recv,
):
    rep = lax.axis_index("rep")
    grp = lax.axis_index("grp")
    x_lo = grp // 32
    z = (grp // 2) % NZ
    core = grp % 2
    partner = grp + 1 - 2 * core
    beside = grp + 32 - 64 * x_lo

    def along(d):
        return lax.rem(z + (d + NZ), NZ)

    def at_z(zz):
        return x_lo * 32 + zz * 2 + core

    def rcopy(src, dst, ssem, rsem, r, g):
        return pltpu.make_async_remote_copy(
            src_ref=src, dst_ref=dst, send_sem=ssem, recv_sem=rsem,
            device_id=(r, g), device_id_type=MESH,
        )

    def mate(k):
        return lax.rem(rep + k, REPS)

    barrier = pltpu.get_barrier_semaphore()
    near = [d for s in range(REACH, 0, -1) for d in (s, -s)]
    for k in range(1, REPS):
        pl.semaphore_signal(barrier, inc=1, device_id=(mate(k), grp), device_id_type=MESH)
    for d in near:
        pl.semaphore_signal(barrier, inc=1, device_id=(rep, at_z(along(d))), device_id_type=MESH)
    pl.semaphore_signal(barrier, inc=1, device_id=(rep, partner), device_id_type=MESH)
    pl.semaphore_signal(barrier, inc=1, device_id=(rep, beside), device_id_type=MESH)

    small = [
        pltpu.make_async_copy(src, dst, loc.at[5 + i])
        for i, (src, dst) in enumerate(
            ((wqkv_hbm, wqkv_ref), (wo_hbm, wo_ref), (lab_hbm, lab_ref), (filt_hbm, filt_ref))
        )
    ]
    for c in small:
        c.start()
    window = pl.multiple_of(128 * (3 * rep + rep // 2), 128)
    shift_own = 64 * (rep % 2)
    cnh = pltpu.make_async_copy(noise_hbm.at[0, pl.ds(128, 128)], nhi, loc.at[3])
    cnh.start()
    cnl = pltpu.make_async_copy(
        noise_hbm.at[0, pl.ds(0, 128), :, pl.ds(0, 128)], nband.at[pl.ds(0, 128)], loc.at[4]
    )
    cnl.start()
    cx = pltpu.make_async_copy(x_hbm, xb, loc.at[0])
    cx.start()
    czx = pltpu.make_async_copy(x_hbm, zb, loc.at[1])
    czy = pltpu.make_async_copy(y_hbm, zb, loc.at[1])

    @pl.when(rep < HQ)
    def _():
        czx.start()

    @pl.when(rep >= HQ)
    def _():
        czy.start()

    cy = pltpu.make_async_copy(y_hbm.at[:, pl.ds(window, 512)], yw, loc.at[2])
    cy.start()

    small[0].wait()
    small[1].wait()
    zero_row = jnp.zeros((1, 768), F32)
    wq = jnp.concatenate([wqkv_ref[...].astype(F32), zero_row], axis=0)
    wo = jnp.concatenate([wo_ref[...].astype(F32), zero_row[:, :512]], axis=0)
    lane8 = iota((8, 128), 1)
    slot = rep // 2
    for d in range(REPS):
        if d < HQ:
            chunk, kv = wq[:, 128 * d : 128 * d + 128], wq[:, 512:640]
        else:
            chunk, kv = wo[:, 128 * (d - HQ) : 128 * (d - HQ) + 128], wq[:, 640:768]
        turned = pltpu.roll(kv, lax.rem(32 * slot + 128 - 32 * (d % 4), 128), 1)
        p0s[d, 0] = chunk.astype(BF)
        p0s[d, 1] = jnp.where(lane8 // 32 == slot, turned, 0.0).astype(BF)
    p0r[rep] = p0s[rep]

    pl.semaphore_wait(barrier, len(near) + REPS - 1 + 2)

    for k in range(1, REPS):
        rcopy(p0s.at[mate(k)], p0r.at[rep], p0_send, p0_recv.at[rep], mate(k), grp).start()

    cnh.wait()

    def band(i, carry):
        rows = pl.ds(pl.multiple_of(16 * i, 16), 16)
        low = nhi[rows, :, 0:128].astype(F32)
        high = nhi[rows, :, 128:256].astype(F32)
        keep = iota((16, HQ, 128), 2) > iota((16, HQ, 128), 0) + 16 * i
        nband[pl.ds(pl.multiple_of(128 + 16 * i, 16), 16)] = jnp.where(keep, low, high).astype(BF)
        return carry

    lax.fori_loop(0, 8, band, 0)
    cnl.wait()

    def slice_of(r):
        return nband.at[pl.ds(pl.multiple_of(r * 32, 32), 32)]

    for k in range(1, REPS):
        rcopy(slice_of(mate(k)), nrecv.at[rep], nz_send, nz_recv.at[rep], mate(k), grp).start()
    nrecv[rep] = nband[pl.ds(pl.multiple_of(rep * 32, 32), 32)]

    low, high = (0, 0, 128, 256), (384, 512, 640, 640)
    col = iota((256, 256), 1)
    feature = iota((256, 256), 0)
    part = col % 16
    for b in range(4):
        want = 7 * (16 * b + col // 16) + part % 8
        inside = part % 8 < ROWS
        sel_e[b, 0:256] = jnp.where(inside & (part < 8) & (feature + low[b] == want), 1.0, 0.0).astype(BF)
        sel_e[b, 256:512] = jnp.where(
            inside & (part >= 8) & (feature + high[b] == want + 448), 1.0, 0.0
        ).astype(BF)

    for k in range(1, REPS):
        s = mate(k)
        rcopy(p0s.at[s], p0r.at[s], p0_send, p0_recv.at[s], s, grp).wait_recv()
    for t in range(4):
        wbuf[t, grp, 0:8] = p0r[2 * t, 0]
        wbuf[t, grp, 8:16] = p0r[2 * t + 1, 0]
    for half in range(2):
        total = p0r[half, 1].astype(F32)
        for b in range(1, 4):
            total = total + p0r[2 * b + half, 1].astype(F32)
        wbuf[4, grp, 8 * half : 8 * half + 8] = total.astype(BF)

    def piece(p, g):
        return rcopy(wbuf.at[:, p], wbuf.at[:, p], w_send, w_recv.at[p], rep, g)

    for d in near:
        piece(grp, at_z(along(d))).start()
    piece(grp, beside).start()
    piece(grp, partner).start()

    cx.wait()
    czx.wait()

    def spread(t):
        for b in range(4):
            cols = slice(256 * b, 256 * b + 256)
            for src, dst in ((xb, xe), (zb, ze)):
                lo = dot(src[:, 896 * t + low[b] : 896 * t + low[b] + 256], sel_e[b, 0:256])
                hi = dot(src[:, 896 * t + high[b] : 896 * t + high[b] + 256], sel_e[b, 256:512])
                dst[t, :, cols] = (lo + hi).astype(BF)

    def land(d):
        p = at_z(along(d))
        piece(p, grp).wait_recv()
        return p

    def hand_on(p):
        piece(p, beside).start()
        piece(p, partner).start()

    spread(0)

    p = land(-REACH)
    for s in range(REACH, 0, -1):
        piece(p, at_z(along(s))).start()
    hand_on(p)
    p = land(REACH)
    for s in range(REACH - 1, 0, -1):
        piece(p, at_z(along(-s))).start()
    hand_on(p)
    for s in range(1, REACH):
        hand_on(land(-s))
        hand_on(land(s))

    spread(1)

    for k in range(1, REPS):
        s = mate(k)
        rcopy(slice_of(s), nrecv.at[s], nz_send, nz_recv.at[s], s, grp).wait_recv()
    small[3].wait()
    kept = nrecv[0].astype(F32)
    for s in range(1, REPS):
        kept = jnp.where(filt_ref[0, s] == 1, nrecv[s].astype(F32), kept)
    rows_own = pl.ds(pl.multiple_of(rep * 32, 32), 32)
    for h in range(HQ):
        rows = kept[:, h, :].astype(BF)
        nstage[h] = rows
        nfull[h, rows_own] = rows
    for k in range(1, REPS):
        rcopy(nstage, nfull.at[:, rows_own], nf_send, nf_recv.at[rep], mate(k), grp).start()

    spread(2)
    spread(3)

    for s in range(REACH + 1, 2 * REACH):
        hand_on(land(-s))
        hand_on(land(s))
    hand_on(land(-2 * REACH))

    outward = [0] + [d for s in range(1, 2 * REACH) for d in (-s, s)] + [2 * REACH]
    for d in outward:
        q = (1 - x_lo) * 32 + along(d) * 2 + core
        piece(q, grp).wait_recv()
        piece(q, partner).start()

    def from_partner(side):
        def one(i, carry):
            piece(side * 32 + lax.rem(z + i, NZ) * 2 + 1 - core, grp).wait_recv()
            return carry

        lax.fori_loop(0, NZ, one, 0)

    lane = iota((SEQ, HD), 1) // 32

    def kv_part(side):
        w = wbuf[4, pl.ds(side * 32, 32)].reshape(512, HD)
        lanes = pl.ds(pl.multiple_of(512 * side, 128), 512)
        total = jnp.zeros((SEQ, HD), F32)
        for b in range(4):
            total = jnp.where(lane == b, dot(xe[b, :, lanes], w), total)
        return total

    def own_part(side):
        lanes = pl.ds(pl.multiple_of(512 * side, 128), 512)
        total = jnp.zeros((SEQ, HD), F32)
        for t in range(4):
            total = total + dot(ze[t, :, lanes], wbuf[t, pl.ds(side * 32, 32)].reshape(512, HD))
        return total

    from_partner(x_lo)
    kv_sum = kv_part(x_lo)
    own_cols = own_part(x_lo)
    from_partner(1 - x_lo)
    kv_sum = kv_sum + kv_part(1 - x_lo)
    kv_sum = kv_sum + pltpu.roll(kv_sum, 64, 1)
    kv_sum = kv_sum + pltpu.roll(kv_sum, 32, 1)
    lane64 = iota((64, HD), 1) // 32
    packed = kv_sum[0:64]
    for b in range(1, 4):
        packed = jnp.where(lane64 == b, kv_sum[64 * b : 64 * b + 64], packed)
    kvp[rep] = packed.astype(BF)
    far_first = (2, 6, 1, 3, 5, 7, 4)
    for k in far_first:
        rcopy(kvp.at[rep], kvp.at[rep], kv_send, kv_recv.at[rep], mate(k), grp).start()
    own_cols = own_cols + own_part(1 - x_lo)
    prj[rep] = own_cols.astype(BF)
    for k in (4, 1, 3, 5, 7, 2, 6):
        rcopy(prj.at[rep], prj.at[rep], pr_send, pr_recv.at[rep], mate(k), grp).start()

    crow = iota((512, 128), 0)
    pidx = crow // 8
    owner = ((pidx // 16) % 2) * 32 + (pidx % 16) * 2 + pidx // 32
    want = shift_own + 7 * owner + crow % 8
    want = jnp.where(crow % 8 < ROWS, want, -1)
    for b in range(4):
        own_e[:, 128 * b : 128 * b + 128] = jnp.where(
            iota((512, 128), 1) + 128 * b == want, 1.0, 0.0
        ).astype(BF)
    cy.wait()
    xo_t[...] = dot(own_e[...], xb[:, pl.ds(window, 512)], ((1,), (1,))).astype(BF)
    yo_t[...] = dot(own_e[...], yw[...], ((1,), (1,))).astype(BF)

    small[2].wait()
    lab = lab_ref[...]
    qi, kj = iota((SEQ, SEQ), 0), iota((SEQ, SEQ), 1)
    lab_col = jnp.sum(jnp.where(qi == kj, lab, 0), axis=1, keepdims=True)
    allow[...] = jnp.where((lab_col == lab) & (kj <= qi), 1.0, 0.0)

    for k in range(1, REPS):
        s = mate(k)
        rcopy(kvp.at[s], kvp.at[s], kv_send, kv_recv.at[s], s, grp).wait_recv()
    for which in range(2):
        parts = [kvp[4 * which + r].astype(F32) for r in range(4)]
        for b in range(4):
            whole = jnp.zeros((64, HD), F32)
            for r in range(4):
                turned = parts[r] if r == b else pltpu.roll(parts[r], (32 * (r - b)) % 128, 1)
                whole = jnp.where(lane64 == r, turned, whole)
            kv_ref[which, 64 * b : 64 * b + 64] = whole.astype(BF)
    for k in range(1, REPS):
        s = mate(k)
        rcopy(nstage, nfull.at[:, pl.ds(pl.multiple_of(s * 32, 32), 32)], nf_send, nf_recv.at[s], s, grp).wait_recv()

    scale = 1.0 / jnp.sqrt(jnp.float32(HD))
    keys, vals = kv_ref[0], kv_ref[1]
    key_grad = jnp.zeros((SEQ, HD), F32)
    val_grad = jnp.zeros((SEQ, HD), F32)

    def put(g32, at, product):
        g32[:, :, 128 * at : 128 * at + 128] = product.reshape(PIECES, 8, HD)

    heads = [lax.rem(rep + o, HQ) for o in (0, 1, 3, 2)]

    place = ((g_0, 0), (g_1, 0), (g_1, 2), (g_2, 0))

    def attend(i, key_grad, val_grad):
        h = heads[i]
        if i == 0:
            s = mate(HQ)
            rcopy(prj.at[s], prj.at[s], pr_send, pr_recv.at[s], s, grp).wait_recv()
        else:
            for s in (h, HQ + h):
                rcopy(prj.at[s], prj.at[s], pr_send, pr_recv.at[s], s, grp).wait_recv()
        q, a = prj[h], prj[HQ + h]
        scores = dot(q, keys, ((1,), (1,))) * scale
        scores = jnp.where(allow[...] > 0.5, scores, -jnp.inf)
        expon = jnp.exp(scores - jnp.max(scores, axis=1, keepdims=True))
        probs = expon / jnp.sum(expon, axis=1, keepdims=True)
        factor = 1.0 + nfull[h].astype(F32)
        factor = jnp.concatenate([factor, factor], axis=1)
        dropped = (probs * factor).astype(BF)
        attended = dot(dropped, vals).astype(BF)
        val_grad = val_grad + dot(dropped, a, ((0,), (0,)))
        prob_grad = dot(a, vals, ((1,), (1,))) * factor
        inner = jnp.sum(probs * prob_grad, axis=1, keepdims=True)
        score_grad = (probs * (prob_grad - inner) * scale).astype(BF)
        query_grad = dot(score_grad, keys).astype(BF)
        key_grad = key_grad + dot(score_grad, q, ((0,), (0,)))
        g32, at = place[i]
        put(g32, at, dot(xo_t[...], query_grad))
        put(g32, at + 1, dot(yo_t[...], attended))
        return key_grad, val_grad

    theirs, mine = (1 - core) * 32, core * 32
    order = [2 * REACH] + [d for s in range(2 * REACH - 1, 0, -1) for d in (s, -s)] + [0]

    def relay_at(d):
        return d + REACH - 1 if d < 0 else d + REACH - 2

    def fin_at(d):
        return d + REACH if d < 0 else d + REACH - 1

    class Sums:
        def __init__(self, n, g32, gs, r1, s2, r2, acc, s3, relay, fin):
            self.n, self.g32, self.gs, self.r1, self.s2, self.r2 = n, g32, gs, r1, s2, r2
            self.acc, self.s3, self.relay, self.fin = acc, s3, relay, fin

        def core_copy(self, i):
            return rcopy(self.gs.at[i], self.r1.at[i], r1_send.at[self.n], r1_recv.at[self.n, i], rep, partner)

        def cross(self, zz):
            return rcopy(self.s2.at[zz], self.r2.at[zz], r2_send.at[self.n], r2_recv.at[self.n, zz], rep, beside)

        def hop(self, zz, dst, rsem, d):
            return rcopy(self.s3.at[zz], dst, r3_send.at[self.n], rsem, rep, at_z(along(d)))

        def fin_copy(self, zz, d):
            return self.hop(zz, self.fin.at[fin_at(d)], fin_recv.at[self.n, fin_at(d)], d)

        def relay_copy(self, zz, d):
            return self.hop(zz, self.relay.at[relay_at(d)], relay_recv.at[self.n, relay_at(d)], d)

        def to_partner(self):
            for i in range(2):
                xs = (1 - x_lo) if i == 0 else x_lo
                self.gs[i] = self.g32[pl.ds(theirs + xs * 16, 16)].astype(BF)
                self.core_copy(i).start()

        def to_beside(self):
            self.core_copy(0).wait_recv()
            self.s2[...] = (
                self.g32[pl.ds(mine + (1 - x_lo) * 16, 16)] + self.r1[0].astype(F32)
            ).astype(BF)
            for d in order:
                self.cross(along(d)).start()
            self.core_copy(1).wait_recv()
            self.acc[...] = self.g32[pl.ds(mine + x_lo * 16, 16)] + self.r1[1].astype(F32)

        def to_z(self):
            for d in order:
                zz = along(d)
                self.cross(zz).wait_recv()
                total = self.acc[zz] + self.r2[zz].astype(F32)
                if d == 0 or abs(d) == REACH:
                    self.acc[zz] = total
                    continue
                self.s3[zz] = total.astype(BF)
                if abs(d) > REACH:
                    self.relay_copy(zz, d - REACH if d > 0 else d + REACH).start()
                else:
                    self.fin_copy(zz, d).start()

        def relays(self):
            for sign in (1, -1):
                zz = along(sign * REACH)
                total = self.acc[zz]
                for s in range(REACH if sign > 0 else REACH - 1, 0, -1):
                    self.relay_copy(zz, sign * s).wait_recv()
                    total = total + self.relay[relay_at(sign * s)].astype(F32)
                self.s3[zz] = total.astype(BF)
                self.fin_copy(zz, sign * REACH).start()

        def final(self):
            total = self.acc[z]
            for s in range(1, REACH + 1):
                for d in (s, -s):
                    self.fin_copy(z, d).wait_recv()
                    total = total + self.fin[fin_at(d)].astype(F32)
            return total

    one = Sums(0, g_0, gs_0, r1_0, s2_0, r2_0, acc_0, s3_0, relay_0, fin_0)
    two = Sums(1, g_1, gs_1, r1_1, s2_1, r2_1, acc_1, s3_1, relay_1, fin_1)
    three = Sums(2, g_2, gs_2, r1_2, s2_2, r2_2, acc_2, s3_2, relay_2, fin_2)

    key_grad, val_grad = attend(0, key_grad, val_grad)
    one.to_partner()
    key_grad, val_grad = attend(1, key_grad, val_grad)
    one.to_beside()
    key_grad, val_grad = attend(2, key_grad, val_grad)
    two.to_partner()
    one.to_z()
    two.to_beside()
    key_grad, val_grad = attend(3, key_grad, val_grad)
    put(g_2, 2, dot(xo_t[...], key_grad.astype(BF)))
    put(g_2, 3, dot(xo_t[...], val_grad.astype(BF)))
    three.to_partner()
    two.to_z()
    three.to_beside()
    one.relays()
    three.to_z()
    two.relays()
    three.relays()

    def write(total, at, lanes):
        out_ref[:, lanes] = total[0:ROWS, 128 * at : 128 * at + 128]

    finals = {id(g.g32): g.final() for g in (one, two, three)}
    for i, (g32, at) in enumerate(place):
        write(finals[id(g32)], at, pl.ds(pl.multiple_of(128 * heads[i], 128), 128))
        write(finals[id(g32)], at + 1, pl.ds(pl.multiple_of(768 + 128 * heads[i], 128), 128))
    write(finals[id(g_2)], 2, pl.ds(512, 128))
    write(finals[id(g_2)], 3, pl.ds(640, 128))

    def sent(ref, sem):
        pltpu.make_async_copy(ref, ref, sem).wait()

    sent(p0s.at[pl.ds(0, 7)], p0_send)
    sent(nrecv.at[pl.ds(0, 7)], nz_send)
    for k in range(1, REPS):
        rcopy(nstage, nfull.at[:, rows_own], nf_send, nf_recv.at[rep], mate(k), grp).wait_send()
    sent(wbuf.at[:, pl.ds(0, 63)], w_send)
    sent(kvp.at[pl.ds(0, 7)], kv_send)
    sent(prj.at[pl.ds(0, 7)], pr_send)
    for g in (one, two, three):
        sent(g.gs, r1_send.at[g.n])
        sent(g.s2, r2_send.at[g.n])
        sent(g.s3.at[pl.ds(0, 15)], r3_send.at[g.n])


def per_device(x, y, wqkv, wo, lab, noise, filt):
    vm = pltpu.VMEM
    dma = pltpu.SemaphoreType.DMA
    vspec = pl.BlockSpec(memory_space=pltpu.VMEM)
    anys = pl.BlockSpec(memory_space=pl.ANY)
    return pl.pallas_call(
        kernel,
        out_shape=pltpu.VMEM((ROWS, OUTC), F32),
        in_specs=[anys] * 7,
        out_specs=vspec,
        scratch_shapes=[
            vm((ROWS, 768), BF),
            vm((ROWS, 512), BF),
            vm((1, SEQ), jnp.int32),
            pltpu.SMEM((1, REPS), jnp.int32),
            vm((SEQ, D), BF),
            vm((SEQ, D), BF),
            vm((SEQ, 512), BF),
            vm((4, 512, 256), BF),
            vm((512, 512), BF),
            vm((4, SEQ, 1024), BF),
            vm((4, SEQ, 1024), BF),
            vm((512, SEQ), BF),
            vm((512, SEQ), BF),
            vm((REPS, 2, 8, 128), BF),
            vm((REPS, 2, 8, 128), BF),
            vm((5, PIECES, 16, 128), BF),
            vm((128, HQ, SEQ), BF),
            vm((SEQ, HQ, 128), BF),
            vm((REPS, 32, HQ, 128), BF),
            vm((HQ, 32, 128), BF),
            vm((HQ, SEQ, 128), BF),
            vm((REPS, SEQ, HD), BF),
            vm((REPS, 64, HD), BF),
            vm((2, SEQ, HD), BF),
            vm((SEQ, SEQ), F32),
        ]
        + [
            s
            for width in (256, 512, 512)
            for s in (
                vm((PIECES, 8, width), F32),
                vm((2, NZ, 8, width), BF),
                vm((2, NZ, 8, width), BF),
                vm((NZ, 8, width), BF),
                vm((NZ, 8, width), BF),
                vm((NZ, 8, width), F32),
                vm((NZ, 8, width), BF),
                vm((2 * REACH - 1, 8, width), BF),
                vm((2 * REACH, 8, width), BF),
            )
        ]
        + [
            dma((9,)),
            dma, dma((REPS,)),
            dma, dma((REPS,)),
            dma, dma((REPS,)),
            dma, dma((PIECES,)),
            dma, dma((REPS,)),
            dma, dma((REPS,)),
            dma((3,)), dma((3, 2)),
            dma((3,)), dma((3, NZ)),
            dma((3,)), dma((3, 2 * REACH - 1)), dma((3, 2 * REACH)),
        ],
        compiler_params=pltpu.CompilerParams(
            collective_id=0, has_side_effects=True, vmem_limit_bytes=56 * 1024 * 1024
        ),
    )(x, y, wqkv, wo, lab, noise, filt.reshape(1, REPS))


def solution(mesh):
    return jax.shard_map(
        per_device,
        mesh=mesh,
        in_specs=(
            P("grp", None),
            P("grp", None),
            P(("rep", "grp"), None),
            P(("rep", "grp"), None),
            P("grp", None),
            P("rep", "grp", None, None),
            P(None, "grp"),
        ),
        out_specs=P(("rep", "grp"), None),
        check_vma=False,
    )
```

```python
import functools

import jax
import jax.numpy as jnp
from jax import lax
from jax.experimental import pallas as pl
from jax.experimental.pallas import tpu as pltpu
from jax.sharding import PartitionSpec as P

MESH = pl.DeviceIdType.MESH
BF = jnp.bfloat16
F32 = jnp.float32
REPS = 8
NZ = 16
PIECES = 64
REACH = 4
SEQ = 256
D = 3584
HD = 128
HQ = 4
ROWS = 7
OUTC = 1280


def iota(shape, dim):
    return lax.broadcasted_iota(jnp.int32, shape, dim)


def dot(a, b, dims=((1,), (0,))):
    return lax.dot_general(a, b, (dims, ((), ())), preferred_element_type=F32)


def kernel(
    x_hbm, y_hbm, wqkv_hbm, wo_hbm, lab_hbm, noise_hbm, filt_hbm,
    out_ref, wqkv_ref, wo_ref, lab_ref, filt_ref,
    xb, zb, yw, sel_e, own_e, xe, ze, xo_t, yo_t, p0s, p0r, wbuf,
    nhi, nband, nrecv, nstage, nfull, prj, kvp, kv_ref, allow,
    g_0, gs_0, r1_0, s2_0, r2_0, acc_0, s3_0, relay_0, fin_0,
    g_1, gs_1, r1_1, s2_1, r2_1, acc_1, s3_1, relay_1, fin_1,
    loc, p0_send, p0_recv, nz_send, nz_recv, nf_send, nf_recv, w_send, w_recv,
    kv_send, kv_recv, pr_send, pr_recv,
    r1_send, r1_recv, r2_send, r2_recv, r3_send, relay_recv, fin_recv,
):
    rep = lax.axis_index("rep")
    grp = lax.axis_index("grp")
    x_lo = grp // 32
    z = (grp // 2) % NZ
    core = grp % 2
    partner = grp + 1 - 2 * core
    beside = grp + 32 - 64 * x_lo

    way = 1 - 2 * core

    def along(d):
        return lax.rem(z + way * d + NZ, NZ)

    def at_z(zz):
        return x_lo * 32 + zz * 2 + core

    def rcopy(src, dst, ssem, rsem, r, g):
        return pltpu.make_async_remote_copy(
            src_ref=src, dst_ref=dst, send_sem=ssem, recv_sem=rsem,
            device_id=(r, g), device_id_type=MESH,
        )

    def mate(k):
        return lax.rem(rep + k, REPS)

    barrier = pltpu.get_barrier_semaphore()
    near = [d for s in range(REACH, 0, -1) for d in (s, -s)]
    for k in range(1, REPS):
        pl.semaphore_signal(barrier, inc=1, device_id=(mate(k), grp), device_id_type=MESH)
    for d in near:
        pl.semaphore_signal(barrier, inc=1, device_id=(rep, at_z(along(d))), device_id_type=MESH)
    pl.semaphore_signal(barrier, inc=1, device_id=(rep, partner), device_id_type=MESH)
    pl.semaphore_signal(barrier, inc=1, device_id=(rep, beside), device_id_type=MESH)

    small = [
        pltpu.make_async_copy(src, dst, loc.at[5 + i])
        for i, (src, dst) in enumerate(
            ((wqkv_hbm, wqkv_ref), (wo_hbm, wo_ref), (lab_hbm, lab_ref), (filt_hbm, filt_ref))
        )
    ]
    for c in small:
        c.start()
    window = pl.multiple_of(128 * (3 * rep + rep // 2), 128)
    shift_own = 64 * (rep % 2)
    cnh = pltpu.make_async_copy(noise_hbm.at[0, pl.ds(128, 128)], nhi, loc.at[3])
    cnh.start()
    cnl = pltpu.make_async_copy(
        noise_hbm.at[0, pl.ds(0, 128), :, pl.ds(0, 128)], nband.at[pl.ds(0, 128)], loc.at[4]
    )
    cnl.start()
    cx = pltpu.make_async_copy(x_hbm, xb, loc.at[0])
    cx.start()
    czx = pltpu.make_async_copy(x_hbm, zb, loc.at[1])
    czy = pltpu.make_async_copy(y_hbm, zb, loc.at[1])

    @pl.when(rep < HQ)
    def _():
        czx.start()

    @pl.when(rep >= HQ)
    def _():
        czy.start()

    cy = pltpu.make_async_copy(y_hbm.at[:, pl.ds(window, 512)], yw, loc.at[2])
    cy.start()

    small[0].wait()
    small[1].wait()
    zero_row = jnp.zeros((1, 768), F32)
    wq = jnp.concatenate([wqkv_ref[...].astype(F32), zero_row], axis=0)
    wo = jnp.concatenate([wo_ref[...].astype(F32), zero_row[:, :512]], axis=0)
    lane8 = iota((8, 128), 1)
    slot = rep // 2
    for d in range(REPS):
        if d < HQ:
            chunk, kv = wq[:, 128 * d : 128 * d + 128], wq[:, 512:640]
        else:
            chunk, kv = wo[:, 128 * (d - HQ) : 128 * (d - HQ) + 128], wq[:, 640:768]
        turned = pltpu.roll(kv, lax.rem(32 * slot + 128 - 32 * (d % 4), 128), 1)
        p0s[d, 0] = chunk.astype(BF)
        p0s[d, 1] = jnp.where(lane8 // 32 == slot, turned, 0.0).astype(BF)
    p0r[rep] = p0s[rep]

    pl.semaphore_wait(barrier, len(near) + REPS - 1 + 2)

    for k in range(1, REPS):
        rcopy(p0s.at[mate(k)], p0r.at[rep], p0_send, p0_recv.at[rep], mate(k), grp).start()

    cnh.wait()

    def band(i, carry):
        rows = pl.ds(pl.multiple_of(16 * i, 16), 16)
        low = nhi[rows, :, 0:128].astype(F32)
        high = nhi[rows, :, 128:256].astype(F32)
        keep = iota((16, HQ, 128), 2) > iota((16, HQ, 128), 0) + 16 * i
        nband[pl.ds(pl.multiple_of(128 + 16 * i, 16), 16)] = jnp.where(keep, low, high).astype(BF)
        return carry

    lax.fori_loop(0, 8, band, 0)
    cnl.wait()

    def slice_of(r):
        return nband.at[pl.ds(pl.multiple_of(r * 32, 32), 32)]

    for k in range(1, REPS):
        rcopy(slice_of(mate(k)), nrecv.at[rep], nz_send, nz_recv.at[rep], mate(k), grp).start()
    nrecv[rep] = nband[pl.ds(pl.multiple_of(rep * 32, 32), 32)]

    low, high = (0, 0, 128, 256), (384, 512, 640, 640)
    col = iota((256, 256), 1)
    feature = iota((256, 256), 0)
    part = col % 16
    for b in range(4):
        want = 7 * (16 * b + col // 16) + part % 8
        inside = part % 8 < ROWS
        sel_e[b, 0:256] = jnp.where(inside & (part < 8) & (feature + low[b] == want), 1.0, 0.0).astype(BF)
        sel_e[b, 256:512] = jnp.where(
            inside & (part >= 8) & (feature + high[b] == want + 448), 1.0, 0.0
        ).astype(BF)

    for k in range(1, REPS):
        s = mate(k)
        rcopy(p0s.at[s], p0r.at[s], p0_send, p0_recv.at[s], s, grp).wait_recv()
    for t in range(4):
        wbuf[grp, t, 0:8] = p0r[2 * t, 0]
        wbuf[grp, t, 8:16] = p0r[2 * t + 1, 0]
    for half in range(2):
        total = p0r[half, 1].astype(F32)
        for b in range(1, 4):
            total = total + p0r[2 * b + half, 1].astype(F32)
        wbuf[grp, 4, 8 * half : 8 * half + 8] = total.astype(BF)

    def piece(p, g):
        return rcopy(wbuf.at[p], wbuf.at[p], w_send, w_recv.at[p], rep, g)

    for d in near:
        piece(grp, at_z(along(d))).start()
    piece(grp, beside).start()
    piece(grp, partner).start()

    cx.wait()
    czx.wait()

    def spread(t):
        for b in range(4):
            cols = slice(256 * b, 256 * b + 256)
            for src, dst in ((xb, xe), (zb, ze)):
                lo = dot(src[:, 896 * t + low[b] : 896 * t + low[b] + 256], sel_e[b, 0:256])
                hi = dot(src[:, 896 * t + high[b] : 896 * t + high[b] + 256], sel_e[b, 256:512])
                dst[t, :, cols] = (lo + hi).astype(BF)

    def land(d):
        p = at_z(along(d))
        piece(p, grp).wait_recv()
        return p

    def hand_on(p):
        piece(p, beside).start()
        piece(p, partner).start()

    spread(0)

    p = land(-REACH)
    for s in range(REACH, 0, -1):
        piece(p, at_z(along(s))).start()
    hand_on(p)
    p = land(REACH)
    for s in range(REACH - 1, 0, -1):
        piece(p, at_z(along(-s))).start()
    hand_on(p)
    for s in range(1, REACH):
        hand_on(land(-s))
        hand_on(land(s))

    spread(1)

    for k in range(1, REPS):
        s = mate(k)
        rcopy(slice_of(s), nrecv.at[s], nz_send, nz_recv.at[s], s, grp).wait_recv()
    small[3].wait()
    kept = nrecv[0].astype(F32)
    for s in range(1, REPS):
        kept = jnp.where(filt_ref[0, s] == 1, nrecv[s].astype(F32), kept)
    rows_own = pl.ds(pl.multiple_of(rep * 32, 32), 32)
    for h in range(HQ):
        rows = kept[:, h, :].astype(BF)
        nstage[h] = rows
        nfull[h, rows_own] = rows
    for k in range(1, REPS):
        rcopy(nstage, nfull.at[:, rows_own], nf_send, nf_recv.at[rep], mate(k), grp).start()

    spread(2)
    spread(3)

    for s in range(REACH + 1, 2 * REACH):
        hand_on(land(-s))
        hand_on(land(s))
    hand_on(land(-2 * REACH))

    outward = [0] + [d for s in range(1, 2 * REACH) for d in (-s, s)] + [2 * REACH]
    for d in outward:
        q = (1 - x_lo) * 32 + along(d) * 2 + core
        piece(q, grp).wait_recv()
        piece(q, partner).start()

    def from_partner(side):
        def one(i, carry):
            piece(side * 32 + lax.rem(z + i, NZ) * 2 + 1 - core, grp).wait_recv()
            return carry

        lax.fori_loop(0, NZ, one, 0)

    lane = iota((SEQ, HD), 1) // 32

    def kv_part(side):
        w = wbuf[pl.ds(side * 32, 32), 4].reshape(512, HD)
        lanes = pl.ds(pl.multiple_of(512 * side, 128), 512)
        total = jnp.zeros((SEQ, HD), F32)
        for b in range(4):
            total = jnp.where(lane == b, dot(xe[b, :, lanes], w), total)
        return total

    def own_part(side):
        lanes = pl.ds(pl.multiple_of(512 * side, 128), 512)
        total = jnp.zeros((SEQ, HD), F32)
        for t in range(4):
            total = total + dot(ze[t, :, lanes], wbuf[pl.ds(side * 32, 32), t].reshape(512, HD))
        return total

    from_partner(x_lo)
    kv_sum = kv_part(x_lo)
    own_cols = own_part(x_lo)
    from_partner(1 - x_lo)
    kv_sum = kv_sum + kv_part(1 - x_lo)
    kv_sum = kv_sum + pltpu.roll(kv_sum, 64, 1)
    kv_sum = kv_sum + pltpu.roll(kv_sum, 32, 1)
    lane64 = iota((64, HD), 1) // 32
    packed = kv_sum[0:64]
    for b in range(1, 4):
        packed = jnp.where(lane64 == b, kv_sum[64 * b : 64 * b + 64], packed)
    kvp[rep] = packed.astype(BF)
    far_first = (2, 6, 1, 3, 5, 7, 4)
    for k in far_first:
        rcopy(kvp.at[rep], kvp.at[rep], kv_send, kv_recv.at[rep], mate(k), grp).start()
    own_cols = own_cols + own_part(1 - x_lo)
    prj[rep] = own_cols.astype(BF)
    for k in (4, 1, 3, 5, 7, 2, 6):
        rcopy(prj.at[rep], prj.at[rep], pr_send, pr_recv.at[rep], mate(k), grp).start()

    crow = iota((512, 128), 0)
    pidx = crow // 8
    owner = ((pidx // 16) % 2) * 32 + (pidx % 16) * 2 + pidx // 32
    want = shift_own + 7 * owner + crow % 8
    want = jnp.where(crow % 8 < ROWS, want, -1)
    for b in range(4):
        own_e[:, 128 * b : 128 * b + 128] = jnp.where(
            iota((512, 128), 1) + 128 * b == want, 1.0, 0.0
        ).astype(BF)
    cy.wait()
    xo_t[...] = dot(own_e[...], xb[:, pl.ds(window, 512)], ((1,), (1,))).astype(BF)
    yo_t[...] = dot(own_e[...], yw[...], ((1,), (1,))).astype(BF)

    small[2].wait()
    lab = lab_ref[...]
    qi, kj = iota((SEQ, SEQ), 0), iota((SEQ, SEQ), 1)
    lab_col = jnp.sum(jnp.where(qi == kj, lab, 0), axis=1, keepdims=True)
    allow[...] = jnp.where((lab_col == lab) & (kj <= qi), 1.0, 0.0)

    for k in range(1, REPS):
        s = mate(k)
        rcopy(kvp.at[s], kvp.at[s], kv_send, kv_recv.at[s], s, grp).wait_recv()
    for which in range(2):
        parts = [kvp[4 * which + r].astype(F32) for r in range(4)]
        for b in range(4):
            whole = jnp.zeros((64, HD), F32)
            for r in range(4):
                turned = parts[r] if r == b else pltpu.roll(parts[r], (32 * (r - b)) % 128, 1)
                whole = jnp.where(lane64 == r, turned, whole)
            kv_ref[which, 64 * b : 64 * b + 64] = whole.astype(BF)
    for k in range(1, REPS):
        s = mate(k)
        rcopy(nstage, nfull.at[:, pl.ds(pl.multiple_of(s * 32, 32), 32)], nf_send, nf_recv.at[s], s, grp).wait_recv()

    scale = 1.0 / jnp.sqrt(jnp.float32(HD))
    keys, vals = kv_ref[0], kv_ref[1]
    key_grad = jnp.zeros((SEQ, HD), F32)
    val_grad = jnp.zeros((SEQ, HD), F32)

    def put(g32, at, product):
        g32[:, :, 128 * at : 128 * at + 128] = product.reshape(PIECES, 8, HD)

    heads = [lax.rem(rep + o, HQ) for o in (0, 1, 3, 2)]

    place = ((g_0, 0), (g_0, 2), (g_0, 4), (g_1, 0))

    def attend(i, key_grad, val_grad):
        h = heads[i]
        if i == 0:
            s = mate(HQ)
            rcopy(prj.at[s], prj.at[s], pr_send, pr_recv.at[s], s, grp).wait_recv()
        else:
            for s in (h, HQ + h):
                rcopy(prj.at[s], prj.at[s], pr_send, pr_recv.at[s], s, grp).wait_recv()
        q, a = prj[h], prj[HQ + h]
        scores = dot(q, keys, ((1,), (1,))) * scale
        scores = jnp.where(allow[...] > 0.5, scores, -jnp.inf)
        expon = jnp.exp(scores - jnp.max(scores, axis=1, keepdims=True))
        probs = expon / jnp.sum(expon, axis=1, keepdims=True)
        factor = 1.0 + nfull[h].astype(F32)
        factor = jnp.concatenate([factor, factor], axis=1)
        dropped = (probs * factor).astype(BF)
        attended = dot(dropped, vals).astype(BF)
        val_grad = val_grad + dot(dropped, a, ((0,), (0,)))
        prob_grad = dot(a, vals, ((1,), (1,))) * factor
        inner = jnp.sum(probs * prob_grad, axis=1, keepdims=True)
        score_grad = (probs * (prob_grad - inner) * scale).astype(BF)
        query_grad = dot(score_grad, keys).astype(BF)
        key_grad = key_grad + dot(score_grad, q, ((0,), (0,)))
        g32, at = place[i]
        put(g32, at, dot(xo_t[...], query_grad))
        put(g32, at + 1, dot(yo_t[...], attended))
        return key_grad, val_grad

    theirs, mine = (1 - core) * 32, core * 32
    order = [2 * REACH] + [d for s in range(2 * REACH - 1, 0, -1) for d in (s, -s)] + [0]

    def relay_at(d):
        return d + REACH - 1 if d < 0 else d + REACH - 2

    def fin_at(d):
        return d + REACH if d < 0 else d + REACH - 1

    class Sums:
        def __init__(self, n, g32, gs, r1, s2, r2, acc, s3, relay, fin):
            self.n, self.g32, self.gs, self.r1, self.s2, self.r2 = n, g32, gs, r1, s2, r2
            self.acc, self.s3, self.relay, self.fin = acc, s3, relay, fin

        def core_copy(self, i):
            return rcopy(self.gs.at[i], self.r1.at[i], r1_send.at[self.n], r1_recv.at[self.n, i], rep, partner)

        def cross(self, zz):
            return rcopy(self.s2.at[zz], self.r2.at[zz], r2_send.at[self.n], r2_recv.at[self.n, zz], rep, beside)

        def hop(self, zz, dst, rsem, d):
            return rcopy(self.s3.at[zz], dst, r3_send.at[self.n], rsem, rep, at_z(along(d)))

        def fin_copy(self, zz, d):
            return self.hop(zz, self.fin.at[fin_at(d)], fin_recv.at[self.n, fin_at(d)], d)

        def relay_copy(self, zz, d):
            return self.hop(zz, self.relay.at[relay_at(d)], relay_recv.at[self.n, relay_at(d)], d)

        def to_partner(self):
            for i in range(2):
                xs = (1 - x_lo) if i == 0 else x_lo
                self.gs[i] = self.g32[pl.ds(theirs + xs * 16, 16)].astype(BF)
                self.core_copy(i).start()

        def to_beside(self):
            self.core_copy(0).wait_recv()
            self.s2[...] = (
                self.g32[pl.ds(mine + (1 - x_lo) * 16, 16)] + self.r1[0].astype(F32)
            ).astype(BF)
            for d in order:
                self.cross(along(d)).start()
            self.core_copy(1).wait_recv()
            self.acc[...] = self.g32[pl.ds(mine + x_lo * 16, 16)] + self.r1[1].astype(F32)

        def to_z(self):
            for d in order:
                zz = along(d)
                self.cross(zz).wait_recv()
                total = self.acc[zz] + self.r2[zz].astype(F32)
                if d == 0 or abs(d) == REACH:
                    self.acc[zz] = total
                    continue
                self.s3[zz] = total.astype(BF)
                if abs(d) > REACH:
                    self.relay_copy(zz, d - REACH if d > 0 else d + REACH).start()
                else:
                    self.fin_copy(zz, d).start()

        def relays(self):
            for sign in (1, -1):
                zz = along(sign * REACH)
                total = self.acc[zz]
                for s in range(REACH if sign > 0 else REACH - 1, 0, -1):
                    self.relay_copy(zz, sign * s).wait_recv()
                    total = total + self.relay[relay_at(sign * s)].astype(F32)
                self.s3[zz] = total.astype(BF)
                self.fin_copy(zz, sign * REACH).start()

        def final(self):
            total = self.acc[z]
            for s in range(1, REACH + 1):
                for d in (s, -s):
                    self.fin_copy(z, d).wait_recv()
                    total = total + self.fin[fin_at(d)].astype(F32)
            return total

    one = Sums(0, g_0, gs_0, r1_0, s2_0, r2_0, acc_0, s3_0, relay_0, fin_0)
    two = Sums(1, g_1, gs_1, r1_1, s2_1, r2_1, acc_1, s3_1, relay_1, fin_1)
    for i in range(3):
        key_grad, val_grad = attend(i, key_grad, val_grad)
    one.to_partner()
    one.to_beside()
    key_grad, val_grad = attend(3, key_grad, val_grad)
    put(g_1, 2, dot(xo_t[...], key_grad.astype(BF)))
    put(g_1, 3, dot(xo_t[...], val_grad.astype(BF)))
    two.to_partner()
    one.to_z()
    two.to_beside()
    two.to_z()
    one.relays()
    two.relays()

    def write(total, at, lanes):
        out_ref[:, lanes] = total[0:ROWS, 128 * at : 128 * at + 128]

    finals = {id(g.g32): g.final() for g in (one, two)}
    for i, (g32, at) in enumerate(place):
        write(finals[id(g32)], at, pl.ds(pl.multiple_of(128 * heads[i], 128), 128))
        write(finals[id(g32)], at + 1, pl.ds(pl.multiple_of(768 + 128 * heads[i], 128), 128))
    write(finals[id(g_1)], 2, pl.ds(512, 128))
    write(finals[id(g_1)], 3, pl.ds(640, 128))

    def sent(ref, sem):
        pltpu.make_async_copy(ref, ref, sem).wait()

    sent(p0s.at[pl.ds(0, 7)], p0_send)
    sent(nrecv.at[pl.ds(0, 7)], nz_send)
    for k in range(1, REPS):
        rcopy(nstage, nfull.at[:, rows_own], nf_send, nf_recv.at[rep], mate(k), grp).wait_send()
    sent(wbuf.at[pl.ds(0, 63)], w_send)
    sent(kvp.at[pl.ds(0, 7)], kv_send)
    sent(prj.at[pl.ds(0, 7)], pr_send)
    for g in (one, two):
        sent(g.gs, r1_send.at[g.n])
        sent(g.s2, r2_send.at[g.n])
        sent(g.s3.at[pl.ds(0, 15)], r3_send.at[g.n])


def per_device(x, y, wqkv, wo, lab, noise, filt):
    vm = pltpu.VMEM
    dma = pltpu.SemaphoreType.DMA
    vspec = pl.BlockSpec(memory_space=pltpu.VMEM)
    anys = pl.BlockSpec(memory_space=pl.ANY)
    return pl.pallas_call(
        kernel,
        out_shape=pltpu.VMEM((ROWS, OUTC), F32),
        in_specs=[anys] * 7,
        out_specs=vspec,
        scratch_shapes=[
            vm((ROWS, 768), BF),
            vm((ROWS, 512), BF),
            vm((1, SEQ), jnp.int32),
            pltpu.SMEM((1, REPS), jnp.int32),
            vm((SEQ, D), BF),
            vm((SEQ, D), BF),
            vm((SEQ, 512), BF),
            vm((4, 512, 256), BF),
            vm((512, 512), BF),
            vm((4, SEQ, 1024), BF),
            vm((4, SEQ, 1024), BF),
            vm((512, SEQ), BF),
            vm((512, SEQ), BF),
            vm((REPS, 2, 8, 128), BF),
            vm((REPS, 2, 8, 128), BF),
            vm((PIECES, 5, 16, 128), BF),
            vm((128, HQ, SEQ), BF),
            vm((SEQ, HQ, 128), BF),
            vm((REPS, 32, HQ, 128), BF),
            vm((HQ, 32, 128), BF),
            vm((HQ, SEQ, 128), BF),
            vm((REPS, SEQ, HD), BF),
            vm((REPS, 64, HD), BF),
            vm((2, SEQ, HD), BF),
            vm((SEQ, SEQ), F32),
        ]
        + [
            s
            for width in (768, 512)
            for s in (
                vm((PIECES, 8, width), F32),
                vm((2, NZ, 8, width), BF),
                vm((2, NZ, 8, width), BF),
                vm((NZ, 8, width), BF),
                vm((NZ, 8, width), BF),
                vm((NZ, 8, width), F32),
                vm((NZ, 8, width), BF),
                vm((2 * REACH - 1, 8, width), BF),
                vm((2 * REACH, 8, width), BF),
            )
        ]
        + [
            dma((9,)),
            dma, dma((REPS,)),
            dma, dma((REPS,)),
            dma, dma((REPS,)),
            dma, dma((PIECES,)),
            dma, dma((REPS,)),
            dma, dma((REPS,)),
            dma((2,)), dma((2, 2)),
            dma((2,)), dma((2, NZ)),
            dma((2,)), dma((2, 2 * REACH - 1)), dma((2, 2 * REACH)),
        ],
        compiler_params=pltpu.CompilerParams(
            collective_id=0, has_side_effects=True, vmem_limit_bytes=56 * 1024 * 1024
        ),
    )(x, y, wqkv, wo, lab, noise, filt.reshape(1, REPS))


def solution(mesh):
    return jax.shard_map(
        per_device,
        mesh=mesh,
        in_specs=(
            P("grp", None),
            P("grp", None),
            P(("rep", "grp"), None),
            P(("rep", "grp"), None),
            P("grp", None),
            P("rep", "grp", None, None),
            P(None, "grp"),
        ),
        out_specs=P(("rep", "grp"), None),
        check_vma=False,
    )
```

```python
import functools

import jax
import jax.numpy as jnp
from jax import lax
from jax.experimental import pallas as pl
from jax.experimental.pallas import tpu as pltpu
from jax.sharding import PartitionSpec as P

MESH = pl.DeviceIdType.MESH
BF = jnp.bfloat16
F32 = jnp.float32
REPS = 8
NZ = 16
PIECES = 64
REACH = 4
SEQ = 256
D = 3584
HD = 128
HQ = 4
ROWS = 7
OUTC = 1280


def iota(shape, dim):
    return lax.broadcasted_iota(jnp.int32, shape, dim)


def dot(a, b, dims=((1,), (0,))):
    return lax.dot_general(a, b, (dims, ((), ())), preferred_element_type=F32)


def kernel(
    x_hbm, y_hbm, wqkv_hbm, wo_hbm, lab_hbm, noise_hbm, filt_hbm,
    out_ref, wqkv_ref, wo_ref, lab_ref, filt_ref,
    xb, zb, yw, sel_e, own_e, xe, ze, xo_t, yo_t, p0s, p0r, wbuf,
    nhi, nband, nrecv, nstage, nfull, prj, kvp, kv_ref, allow,
    g_0, gs_0, r1_0, s2_0, r2_0, acc_0, s3_0, relay_0, fin_0,
    g_1, gs_1, r1_1, s2_1, r2_1, acc_1, s3_1, relay_1, fin_1,
    loc, p0_send, p0_recv, nz_send, nz_recv, nf_send, nf_recv, w_send, w_recv,
    kv_send, kv_recv, pr_send, pr_recv,
    r1_send, r1_recv, r2_send, r2_recv, r3_send, relay_recv, fin_recv,
):
    rep = lax.axis_index("rep")
    grp = lax.axis_index("grp")
    x_lo = grp // 32
    z = (grp // 2) % NZ
    core = grp % 2
    partner = grp + 1 - 2 * core
    beside = grp + 32 - 64 * x_lo

    way = 1 - 2 * core

    def along(d):
        return lax.rem(z + way * d + NZ, NZ)

    def at_z(zz):
        return x_lo * 32 + zz * 2 + core

    def rcopy(src, dst, ssem, rsem, r, g):
        return pltpu.make_async_remote_copy(
            src_ref=src, dst_ref=dst, send_sem=ssem, recv_sem=rsem,
            device_id=(r, g), device_id_type=MESH,
        )

    def mate(k):
        return lax.rem(rep + k, REPS)

    barrier = pltpu.get_barrier_semaphore()
    near = [d for s in range(REACH, 0, -1) for d in (s, -s)]
    for k in range(1, REPS):
        pl.semaphore_signal(barrier, inc=1, device_id=(mate(k), grp), device_id_type=MESH)
    for d in near:
        pl.semaphore_signal(barrier, inc=1, device_id=(rep, at_z(along(d))), device_id_type=MESH)
    pl.semaphore_signal(barrier, inc=1, device_id=(rep, partner), device_id_type=MESH)
    pl.semaphore_signal(barrier, inc=1, device_id=(rep, beside), device_id_type=MESH)

    small = [
        pltpu.make_async_copy(src, dst, loc.at[5 + i])
        for i, (src, dst) in enumerate(
            ((wqkv_hbm, wqkv_ref), (wo_hbm, wo_ref), (lab_hbm, lab_ref), (filt_hbm, filt_ref))
        )
    ]
    for c in small:
        c.start()
    window = pl.multiple_of(128 * (3 * rep + rep // 2), 128)
    shift_own = 64 * (rep % 2)
    cnh = pltpu.make_async_copy(noise_hbm.at[0, pl.ds(128, 128)], nhi, loc.at[3])
    cnh.start()
    cnl = pltpu.make_async_copy(
        noise_hbm.at[0, pl.ds(0, 128), :, pl.ds(0, 128)], nband.at[pl.ds(0, 128)], loc.at[4]
    )
    cnl.start()
    cx = pltpu.make_async_copy(x_hbm, xb, loc.at[0])
    cx.start()
    czx = pltpu.make_async_copy(x_hbm, zb, loc.at[1])
    czy = pltpu.make_async_copy(y_hbm, zb, loc.at[1])

    @pl.when(rep < HQ)
    def _():
        czx.start()

    @pl.when(rep >= HQ)
    def _():
        czy.start()

    cy = pltpu.make_async_copy(y_hbm.at[:, pl.ds(window, 512)], yw, loc.at[2])
    cy.start()

    small[0].wait()
    small[1].wait()
    zero_row = jnp.zeros((1, 768), F32)
    wq = jnp.concatenate([wqkv_ref[...].astype(F32), zero_row], axis=0)
    wo = jnp.concatenate([wo_ref[...].astype(F32), zero_row[:, :512]], axis=0)
    lane8 = iota((8, 128), 1)
    slot = rep // 2
    for d in range(REPS):
        if d < HQ:
            chunk, kv = wq[:, 128 * d : 128 * d + 128], wq[:, 512:640]
        else:
            chunk, kv = wo[:, 128 * (d - HQ) : 128 * (d - HQ) + 128], wq[:, 640:768]
        turned = pltpu.roll(kv, lax.rem(32 * slot + 128 - 32 * (d % 4), 128), 1)
        p0s[d, 0] = chunk.astype(BF)
        p0s[d, 1] = jnp.where(lane8 // 32 == slot, turned, 0.0).astype(BF)
    p0r[rep] = p0s[rep]

    pl.semaphore_wait(barrier, len(near) + REPS - 1 + 2)

    for k in range(1, REPS):
        rcopy(p0s.at[mate(k)], p0r.at[rep], p0_send, p0_recv.at[rep], mate(k), grp).start()

    cnh.wait()

    def band(i, carry):
        rows = pl.ds(pl.multiple_of(16 * i, 16), 16)
        low = nhi[rows, :, 0:128].astype(F32)
        high = nhi[rows, :, 128:256].astype(F32)
        keep = iota((16, HQ, 128), 2) > iota((16, HQ, 128), 0) + 16 * i
        nband[pl.ds(pl.multiple_of(128 + 16 * i, 16), 16)] = jnp.where(keep, low, high).astype(BF)
        return carry

    lax.fori_loop(0, 8, band, 0)
    cnl.wait()

    def slice_of(r):
        return nband.at[pl.ds(pl.multiple_of(r * 32, 32), 32)]

    for k in range(1, REPS):
        rcopy(slice_of(mate(k)), nrecv.at[rep], nz_send, nz_recv.at[rep], mate(k), grp).start()
    nrecv[rep] = nband[pl.ds(pl.multiple_of(rep * 32, 32), 32)]

    low, high = (0, 0, 128, 256), (384, 512, 640, 640)
    col = iota((256, 256), 1)
    feature = iota((256, 256), 0)
    part = col % 16
    for b in range(4):
        want = 7 * (16 * b + col // 16) + part % 8
        inside = part % 8 < ROWS
        sel_e[b, 0:256] = jnp.where(inside & (part < 8) & (feature + low[b] == want), 1.0, 0.0).astype(BF)
        sel_e[b, 256:512] = jnp.where(
            inside & (part >= 8) & (feature + high[b] == want + 448), 1.0, 0.0
        ).astype(BF)

    for k in range(1, REPS):
        s = mate(k)
        rcopy(p0s.at[s], p0r.at[s], p0_send, p0_recv.at[s], s, grp).wait_recv()
    for t in range(4):
        wbuf[grp, t, 0:8] = p0r[2 * t, 0]
        wbuf[grp, t, 8:16] = p0r[2 * t + 1, 0]
    for half in range(2):
        total = p0r[half, 1].astype(F32)
        for b in range(1, 4):
            total = total + p0r[2 * b + half, 1].astype(F32)
        wbuf[grp, 4, 8 * half : 8 * half + 8] = total.astype(BF)

    def piece(p, g):
        return rcopy(wbuf.at[p], wbuf.at[p], w_send, w_recv.at[p], rep, g)

    for d in near:
        piece(grp, at_z(along(d))).start()
    piece(grp, beside).start()
    piece(grp, partner).start()

    cx.wait()
    czx.wait()

    def spread(t):
        for b in range(4):
            cols = slice(256 * b, 256 * b + 256)
            for src, dst in ((xb, xe), (zb, ze)):
                lo = dot(src[:, 896 * t + low[b] : 896 * t + low[b] + 256], sel_e[b, 0:256])
                hi = dot(src[:, 896 * t + high[b] : 896 * t + high[b] + 256], sel_e[b, 256:512])
                dst[t, :, cols] = (lo + hi).astype(BF)

    def land(d):
        p = at_z(along(d))
        piece(p, grp).wait_recv()
        return p

    def hand_on(p):
        piece(p, beside).start()
        piece(p, partner).start()

    spread(0)

    p = land(-REACH)
    for s in range(REACH, 0, -1):
        piece(p, at_z(along(s))).start()
    hand_on(p)
    p = land(REACH)
    for s in range(REACH - 1, 0, -1):
        piece(p, at_z(along(-s))).start()
    hand_on(p)
    for s in range(1, REACH):
        hand_on(land(-s))
        hand_on(land(s))

    spread(1)

    for k in range(1, REPS):
        s = mate(k)
        rcopy(slice_of(s), nrecv.at[s], nz_send, nz_recv.at[s], s, grp).wait_recv()
    small[3].wait()
    kept = nrecv[0].astype(F32)
    for s in range(1, REPS):
        kept = jnp.where(filt_ref[0, s] == 1, nrecv[s].astype(F32), kept)
    rows_own = pl.ds(pl.multiple_of(rep * 32, 32), 32)
    for h in range(HQ):
        rows = kept[:, h, :].astype(BF)
        nstage[h] = rows
        nfull[h, rows_own] = rows
    for k in range(1, REPS):
        rcopy(nstage, nfull.at[:, rows_own], nf_send, nf_recv.at[rep], mate(k), grp).start()

    spread(2)
    spread(3)

    for s in range(REACH + 1, 2 * REACH):
        hand_on(land(-s))
        hand_on(land(s))
    hand_on(land(-2 * REACH))

    outward = [0] + [d for s in range(1, 2 * REACH) for d in (-s, s)] + [2 * REACH]
    for d in outward:
        q = (1 - x_lo) * 32 + along(d) * 2 + core
        piece(q, grp).wait_recv()
        piece(q, partner).start()

    def from_partner(side):
        def one(i, carry):
            piece(side * 32 + lax.rem(z + i, NZ) * 2 + 1 - core, grp).wait_recv()
            return carry

        lax.fori_loop(0, NZ, one, 0)

    lane = iota((SEQ, HD), 1) // 32

    def kv_part(side):
        w = wbuf[pl.ds(side * 32, 32), 4].reshape(512, HD)
        lanes = pl.ds(pl.multiple_of(512 * side, 128), 512)
        total = jnp.zeros((SEQ, HD), F32)
        for b in range(4):
            total = jnp.where(lane == b, dot(xe[b, :, lanes], w), total)
        return total

    def own_part(side, rows):
        lanes = pl.ds(pl.multiple_of(512 * side, 128), 512)
        total = jnp.zeros((rows.stop - rows.start, HD), F32)
        for t in range(4):
            total = total + dot(ze[t, rows, lanes], wbuf[pl.ds(side * 32, 32), t].reshape(512, HD))
        return total

    from_partner(x_lo)
    kv_sum = kv_part(x_lo)
    own_cols = own_part(x_lo, slice(0, SEQ))
    from_partner(1 - x_lo)
    kv_sum = kv_sum + kv_part(1 - x_lo)
    kv_sum = kv_sum + pltpu.roll(kv_sum, 64, 1)
    kv_sum = kv_sum + pltpu.roll(kv_sum, 32, 1)
    lane64 = iota((64, HD), 1) // 32
    packed = kv_sum[0:64]
    for b in range(1, 4):
        packed = jnp.where(lane64 == b, kv_sum[64 * b : 64 * b + 64], packed)
    kvp[rep] = packed.astype(BF)
    far_first = (2, 6, 1, 3, 5, 7, 4)
    for k in far_first:
        rcopy(kvp.at[rep], kvp.at[rep], kv_send, kv_recv.at[rep], mate(k), grp).start()
    def columns(r, half, g):
        rows = prj.at[r, pl.ds(128 * half, 128)]
        return rcopy(rows, rows, pr_send, pr_recv.at[half, r], g, grp)

    for half in range(2):
        rows = slice(128 * half, 128 * half + 128)
        prj[rep, rows] = (own_cols[rows] + own_part(1 - x_lo, rows)).astype(BF)
        for k in (4, 1, 3, 5, 7, 2, 6):
            columns(rep, half, mate(k)).start()

    crow = iota((512, 128), 0)
    pidx = crow // 8
    owner = ((pidx // 16) % 2) * 32 + (pidx % 16) * 2 + pidx // 32
    want = shift_own + 7 * owner + crow % 8
    want = jnp.where(crow % 8 < ROWS, want, -1)
    for b in range(4):
        own_e[:, 128 * b : 128 * b + 128] = jnp.where(
            iota((512, 128), 1) + 128 * b == want, 1.0, 0.0
        ).astype(BF)
    cy.wait()
    xo_t[...] = dot(own_e[...], xb[:, pl.ds(window, 512)], ((1,), (1,))).astype(BF)
    yo_t[...] = dot(own_e[...], yw[...], ((1,), (1,))).astype(BF)

    small[2].wait()
    lab = lab_ref[...]
    qi, kj = iota((SEQ, SEQ), 0), iota((SEQ, SEQ), 1)
    lab_col = jnp.sum(jnp.where(qi == kj, lab, 0), axis=1, keepdims=True)
    allow[...] = jnp.where((lab_col == lab) & (kj <= qi), 1.0, 0.0)

    for k in range(1, REPS):
        s = mate(k)
        rcopy(kvp.at[s], kvp.at[s], kv_send, kv_recv.at[s], s, grp).wait_recv()
    for which in range(2):
        parts = [kvp[4 * which + r].astype(F32) for r in range(4)]
        for b in range(4):
            whole = jnp.zeros((64, HD), F32)
            for r in range(4):
                turned = parts[r] if r == b else pltpu.roll(parts[r], (32 * (r - b)) % 128, 1)
                whole = jnp.where(lane64 == r, turned, whole)
            kv_ref[which, 64 * b : 64 * b + 64] = whole.astype(BF)
    for k in range(1, REPS):
        s = mate(k)
        rcopy(nstage, nfull.at[:, pl.ds(pl.multiple_of(s * 32, 32), 32)], nf_send, nf_recv.at[s], s, grp).wait_recv()

    scale = 1.0 / jnp.sqrt(jnp.float32(HD))
    keys, vals = kv_ref[0], kv_ref[1]
    key_grad = jnp.zeros((SEQ, HD), F32)
    val_grad = jnp.zeros((SEQ, HD), F32)

    def put(g32, at, product):
        g32[:, :, 128 * at : 128 * at + 128] = product.reshape(PIECES, 8, HD)

    heads = [lax.rem(rep + o, HQ) for o in (0, 1, 3, 2)]

    place = ((g_0, 0), (g_0, 2), (g_0, 4), (g_1, 0))

    def attend(i, key_grad, val_grad):
        h = heads[i]
        if i == 0:
            for half in range(2):
                columns(mate(HQ), half, mate(HQ)).wait_recv()
        else:
            for s in (h, HQ + h):
                for half in range(2):
                    columns(s, half, s).wait_recv()
        q, a = prj[h], prj[HQ + h]
        scores = dot(q, keys, ((1,), (1,))) * scale
        scores = jnp.where(allow[...] > 0.5, scores, -jnp.inf)
        expon = jnp.exp(scores - jnp.max(scores, axis=1, keepdims=True))
        probs = expon / jnp.sum(expon, axis=1, keepdims=True)
        factor = 1.0 + nfull[h].astype(F32)
        factor = jnp.concatenate([factor, factor], axis=1)
        dropped = (probs * factor).astype(BF)
        attended = dot(dropped, vals).astype(BF)
        val_grad = val_grad + dot(dropped, a, ((0,), (0,)))
        prob_grad = dot(a, vals, ((1,), (1,))) * factor
        inner = jnp.sum(probs * prob_grad, axis=1, keepdims=True)
        score_grad = (probs * (prob_grad - inner) * scale).astype(BF)
        query_grad = dot(score_grad, keys).astype(BF)
        key_grad = key_grad + dot(score_grad, q, ((0,), (0,)))
        g32, at = place[i]
        put(g32, at, dot(xo_t[...], query_grad))
        put(g32, at + 1, dot(yo_t[...], attended))
        return key_grad, val_grad

    theirs, mine = (1 - core) * 32, core * 32
    order = [2 * REACH] + [d for s in range(2 * REACH - 1, 0, -1) for d in (s, -s)] + [0]

    def relay_at(d):
        return d + REACH - 1 if d < 0 else d + REACH - 2

    def fin_at(d):
        return d + REACH if d < 0 else d + REACH - 1

    class Sums:
        def __init__(self, n, g32, gs, r1, s2, r2, acc, s3, relay, fin):
            self.n, self.g32, self.gs, self.r1, self.s2, self.r2 = n, g32, gs, r1, s2, r2
            self.acc, self.s3, self.relay, self.fin = acc, s3, relay, fin

        def core_copy(self, i):
            return rcopy(self.gs.at[i], self.r1.at[i], r1_send.at[self.n], r1_recv.at[self.n, i], rep, partner)

        def cross(self, zz):
            return rcopy(self.s2.at[zz], self.r2.at[zz], r2_send.at[self.n], r2_recv.at[self.n, zz], rep, beside)

        def hop(self, zz, dst, rsem, d):
            return rcopy(self.s3.at[zz], dst, r3_send.at[self.n], rsem, rep, at_z(along(d)))

        def fin_copy(self, zz, d):
            return self.hop(zz, self.fin.at[fin_at(d)], fin_recv.at[self.n, fin_at(d)], d)

        def relay_copy(self, zz, d):
            return self.hop(zz, self.relay.at[relay_at(d)], relay_recv.at[self.n, relay_at(d)], d)

        def to_partner(self):
            for i in range(2):
                xs = (1 - x_lo) if i == 0 else x_lo
                self.gs[i] = self.g32[pl.ds(theirs + xs * 16, 16)].astype(BF)
                self.core_copy(i).start()

        def to_beside(self):
            self.core_copy(0).wait_recv()
            for d in order:
                zz = along(d)
                self.s2[zz] = (
                    self.g32[mine + (1 - x_lo) * 16 + zz] + self.r1[0, zz].astype(F32)
                ).astype(BF)
                self.cross(zz).start()
            self.core_copy(1).wait_recv()
            self.acc[...] = self.g32[pl.ds(mine + x_lo * 16, 16)] + self.r1[1].astype(F32)

        def to_z(self):
            for d in order:
                zz = along(d)
                self.cross(zz).wait_recv()
                total = self.acc[zz] + self.r2[zz].astype(F32)
                if d == 0 or abs(d) == REACH:
                    self.acc[zz] = total
                    continue
                self.s3[zz] = total.astype(BF)
                if abs(d) > REACH:
                    self.relay_copy(zz, d - REACH if d > 0 else d + REACH).start()
                else:
                    self.fin_copy(zz, d).start()

        def relays(self):
            for sign in (1, -1):
                zz = along(sign * REACH)
                total = self.acc[zz]
                for s in range(REACH if sign > 0 else REACH - 1, 0, -1):
                    self.relay_copy(zz, sign * s).wait_recv()
                    total = total + self.relay[relay_at(sign * s)].astype(F32)
                self.s3[zz] = total.astype(BF)
                self.fin_copy(zz, sign * REACH).start()

        def final(self):
            total = self.acc[z]
            for s in range(1, REACH + 1):
                for d in (s, -s):
                    self.fin_copy(z, d).wait_recv()
                    total = total + self.fin[fin_at(d)].astype(F32)
            return total

    one = Sums(0, g_0, gs_0, r1_0, s2_0, r2_0, acc_0, s3_0, relay_0, fin_0)
    two = Sums(1, g_1, gs_1, r1_1, s2_1, r2_1, acc_1, s3_1, relay_1, fin_1)
    for i in range(3):
        key_grad, val_grad = attend(i, key_grad, val_grad)
    one.to_partner()
    one.to_beside()
    key_grad, val_grad = attend(3, key_grad, val_grad)
    put(g_1, 2, dot(xo_t[...], key_grad.astype(BF)))
    put(g_1, 3, dot(xo_t[...], val_grad.astype(BF)))
    two.to_partner()
    one.to_z()
    two.to_beside()
    two.to_z()
    one.relays()
    two.relays()

    def write(total, at, lanes):
        out_ref[:, lanes] = total[0:ROWS, 128 * at : 128 * at + 128]

    finals = {id(g.g32): g.final() for g in (one, two)}
    for i, (g32, at) in enumerate(place):
        write(finals[id(g32)], at, pl.ds(pl.multiple_of(128 * heads[i], 128), 128))
        write(finals[id(g32)], at + 1, pl.ds(pl.multiple_of(768 + 128 * heads[i], 128), 128))
    write(finals[id(g_1)], 2, pl.ds(512, 128))
    write(finals[id(g_1)], 3, pl.ds(640, 128))

    def sent(ref, sem):
        pltpu.make_async_copy(ref, ref, sem).wait()

    sent(p0s.at[pl.ds(0, 7)], p0_send)
    sent(nrecv.at[pl.ds(0, 7)], nz_send)
    for k in range(1, REPS):
        rcopy(nstage, nfull.at[:, rows_own], nf_send, nf_recv.at[rep], mate(k), grp).wait_send()
    sent(wbuf.at[pl.ds(0, 63)], w_send)
    sent(kvp.at[pl.ds(0, 7)], kv_send)
    sent(prj.at[pl.ds(0, 7)], pr_send)
    for g in (one, two):
        sent(g.gs, r1_send.at[g.n])
        sent(g.s2, r2_send.at[g.n])
        sent(g.s3.at[pl.ds(0, 15)], r3_send.at[g.n])


def per_device(x, y, wqkv, wo, lab, noise, filt):
    vm = pltpu.VMEM
    dma = pltpu.SemaphoreType.DMA
    vspec = pl.BlockSpec(memory_space=pltpu.VMEM)
    anys = pl.BlockSpec(memory_space=pl.ANY)
    return pl.pallas_call(
        kernel,
        out_shape=pltpu.VMEM((ROWS, OUTC), F32),
        in_specs=[anys] * 7,
        out_specs=vspec,
        scratch_shapes=[
            vm((ROWS, 768), BF),
            vm((ROWS, 512), BF),
            vm((1, SEQ), jnp.int32),
            pltpu.SMEM((1, REPS), jnp.int32),
            vm((SEQ, D), BF),
            vm((SEQ, D), BF),
            vm((SEQ, 512), BF),
            vm((4, 512, 256), BF),
            vm((512, 512), BF),
            vm((4, SEQ, 1024), BF),
            vm((4, SEQ, 1024), BF),
            vm((512, SEQ), BF),
            vm((512, SEQ), BF),
            vm((REPS, 2, 8, 128), BF),
            vm((REPS, 2, 8, 128), BF),
            vm((PIECES, 5, 16, 128), BF),
            vm((128, HQ, SEQ), BF),
            vm((SEQ, HQ, 128), BF),
            vm((REPS, 32, HQ, 128), BF),
            vm((HQ, 32, 128), BF),
            vm((HQ, SEQ, 128), BF),
            vm((REPS, SEQ, HD), BF),
            vm((REPS, 64, HD), BF),
            vm((2, SEQ, HD), BF),
            vm((SEQ, SEQ), F32),
        ]
        + [
            s
            for width in (768, 512)
            for s in (
                vm((PIECES, 8, width), F32),
                vm((2, NZ, 8, width), BF),
                vm((2, NZ, 8, width), BF),
                vm((NZ, 8, width), BF),
                vm((NZ, 8, width), BF),
                vm((NZ, 8, width), F32),
                vm((NZ, 8, width), BF),
                vm((2 * REACH - 1, 8, width), BF),
                vm((2 * REACH, 8, width), BF),
            )
        ]
        + [
            dma((9,)),
            dma, dma((REPS,)),
            dma, dma((REPS,)),
            dma, dma((REPS,)),
            dma, dma((PIECES,)),
            dma, dma((REPS,)),
            dma, dma((2, REPS)),
            dma((2,)), dma((2, 2)),
            dma((2,)), dma((2, NZ)),
            dma((2,)), dma((2, 2 * REACH - 1)), dma((2, 2 * REACH)),
        ],
        compiler_params=pltpu.CompilerParams(
            collective_id=0, has_side_effects=True, vmem_limit_bytes=56 * 1024 * 1024
        ),
    )(x, y, wqkv, wo, lab, noise, filt.reshape(1, REPS))


def solution(mesh):
    return jax.shard_map(
        per_device,
        mesh=mesh,
        in_specs=(
            P("grp", None),
            P("grp", None),
            P(("rep", "grp"), None),
            P(("rep", "grp"), None),
            P("grp", None),
            P("rep", "grp", None, None),
            P(None, "grp"),
        ),
        out_specs=P(("rep", "grp"), None),
        check_vma=False,
    )
```
